128 devices in a mesh: vocab: 8 (over x, core), expert: 16 (over y, z).
Axes of the slice: x: 4, y: 4, z: 4, core: 2. Of those that a mesh axis runs over, the one named last changes fastest.
Arguments:
- leading_batch_features: bfloat16 [1024, 2880], P(('vocab', 'expert')), may hold values from -48 to 48
- sampling_heat_selector: int32 [1024], replicated, may hold values from 0 to 3
- output_embedding_matrix: bfloat16 [201088, 2880], P(('vocab', 'expert')), may hold values from -3.354102 to 3.354102
- trailing_batch_features: bfloat16 [1024, 2880], P('expert'), may hold values from -6 to 6
- routed_specialist_choice: int32 [1024, 4], P('expert'), may hold values from 0 to 63, all different within a row; in each aligned block of 64 rows (0 to 63, 64 to 127, ...) at most 8 rows name the same one
- dispatcher_projection: bfloat16 [2880, 64], replicated, may hold values from -13.416408 to 13.416408
- specialist_gating_matrix: bfloat16 [64, 2880, 1440], P('expert', None, 'vocab'), may hold values from -0.109375 to 0.109375
- specialist_raising_matrix: bfloat16 [64, 2880, 1440], P('expert', None, 'vocab'), may hold values from -0.109375 to 0.109375
- expert_lowering_matrix: bfloat16 [64, 1440, 2880], P('expert', 'vocab'), may hold values from -0.15625 to 0.15625
Outputs:
- lexicon_log_probability: float32 [1024, 201088], P(None, ('vocab', 'expert'))
- moe_out: bfloat16 [1024, 2880], P('expert', 'vocab')
The draws below stay inside these ranges and needn't reach their ends.
Inputs may be any that keep to these rules, and one draw needn't show every extreme that they name: `routed_specialist_choice`: in the rows of one index of the expert axis no expert is named more than 8 times, a bound that some block reaches.
All inputs are finite; a program needn't handle non-finite values.
Results may differ from the reference program's by a relative error of at most 0.005.
The reference program's roundings to bfloat16 on the way count: a program that leaves them out, or rounds other values in their place, can miss the bound.
Values may be sent and summed in bfloat16 or wider, within the bound.
A program may use at most 256 MiB of HBM per device.

```python
import math
import jax
import jax.numpy as jnp
import numpy as np
from jax import lax

EMBED_DIMENSION = 2880
FF = 1440
TOPK = 4
TB_DEV = 64
EXPERTS = 64
VOCAB = 201088
LEAD_BATCH_SIZE = 1024
TB = 1024
CAP = 8
N_EXPERT = 16


def draw_leading_batch_features(key, part):
    key_base = jax.random.fold_in(jax.random.fold_in(key, 11), 0)
    normal_part = jnp.clip(jax.random.normal(key_base, (LEAD_BATCH_SIZE, EMBED_DIMENSION), jnp.float32), -6.0, 6.0)
    return normal_part.astype(jnp.bfloat16)


def draw_output_embedding_matrix(key, part):
    key_base, key_scale = jax.random.split(jax.random.fold_in(key, 23))
    normal_part = jnp.clip(jax.random.normal(key_base, (VOCAB, EMBED_DIMENSION), jnp.float32), -6.0, 6.0) * EMBED_DIMENSION ** (-0.5)
    frac_rows = (jnp.arange(VOCAB, dtype=jnp.float32) / VOCAB)[:, None]
    row_scale = 2.0 * jnp.exp(frac_rows * jnp.log(3.0) + jax.random.uniform(key_scale, (VOCAB, 1), jnp.float32, -0.7, 0.7))
    return (normal_part * row_scale).astype(jnp.bfloat16)


def draw_dispatcher_projection(key, part):
    key_base = jax.random.fold_in(jax.random.fold_in(key, 37), 0)
    normal_part = jnp.clip(jax.random.normal(key_base, (EMBED_DIMENSION, EXPERTS), jnp.float32), -6.0, 6.0) * 2.0 * EMBED_DIMENSION ** (-0.5)
    return normal_part.astype(jnp.bfloat16)


def place_ends(result, stream_key, low, top_value):
    spot = [jax.random.randint(jax.random.fold_in(stream_key, axis), (), 0, length) for axis, length in enumerate(result.shape)]
    longest = result.shape.index(max(result.shape))
    beside = spot[:longest] + [(spot[longest] + 1) % result.shape[longest]] + spot[longest + 1:]
    return result.at[tuple(spot)].set(low).at[tuple(beside)].set(top_value)


def level_of(stream_key, extent, cuts, low, largest):
    loudness, own = 1.0, jax.random.fold_in(stream_key, 6)
    for axis_at, blocks in cuts:
        draws = jnp.exp(jax.random.uniform(jax.random.fold_in(own, axis_at), (blocks,), jnp.float32, low / len(cuts), largest / len(cuts)))
        loudness = loudness * jnp.repeat(draws, extent[axis_at] // blocks).reshape([-1 if axis == axis_at else 1 for axis in range(len(extent))])
    return loudness


def deal_out(rng, own, number, rows, number_of, top, most, lean):
    sequence = jax.random.permutation(rng, number_of)
    heavy_load, common = shares(number_of, rows * top, most, lean, True), shares(number_of, rows * top, most, lean, False)
    places = jnp.arange(number_of)

    def named(lengths, rotation):
        used = int((lengths > 0).sum())
        fixed = max(1, used // 4)
        shifted = fixed + (places - fixed + rotation * (used - fixed)) % max(1, number_of - fixed)
        return jnp.zeros((number_of,), jnp.int32).at[sequence[jnp.where(places < fixed, places, shifted)]].set(jnp.asarray(lengths, jnp.int32))

    lengths = jnp.where(number % 4 == 0, named(heavy_load, number // 4), named(common, number - number // 4 - 1))
    mixed = jax.random.permutation(jax.random.fold_in(own, 3), number_of)
    source_of, receiver = mixed[0:number_of // 2 * 2:2], mixed[1:number_of // 2 * 2:2]
    slack = jnp.minimum(lengths[source_of] - 1, most - lengths[receiver]) // 2
    slack = jnp.where((source_of == sequence[0]) | (receiver == sequence[0]) | (lengths[receiver] == 0), 0, jnp.maximum(slack, 0))
    shifted = jax.random.randint(jax.random.fold_in(own, 4), (number_of // 2,), 0, 1 << 20) % (slack + 1)
    lengths = lengths.at[source_of].add(-shifted).at[receiver].add(shifted)
    items = jnp.searchsorted(jnp.cumsum(lengths), jnp.arange(rows * top), side="right").astype(jnp.int32)
    listing = items.reshape(top, rows).T
    listing = listing[jax.random.permutation(jax.random.fold_in(own, 1), rows)]
    rotation = jax.random.randint(jax.random.fold_in(own, 2), (rows, 1), 0, top)
    return jnp.take_along_axis(listing, (jnp.arange(top)[None, :] + rotation) % top, axis=1)


def shares(number_of, total, reach, slope, full):
    weights = [(1 << 20) // math.isqrt(grade ** slope) + 1 for grade in range(1, number_of + 1)]
    largest = reach if full else min(reach, max(-(-total // number_of), total * weights[0] // sum(weights)))
    least = 1 if total - largest >= number_of - 1 else 0
    given, surplus = [largest] + [least] * (number_of - 1), total - largest - least * (number_of - 1)
    while surplus > 0:
        candidates = [i for i in range(1, number_of) if given[i] < largest] or [i for i in range(1, number_of) if given[i] < reach]
        whole, left = sum([weights[i] for i in candidates]), surplus
        for i in candidates:
            addition = min(reach - given[i], max(1, left * weights[i] // whole), surplus)
            given[i] = given[i] + addition
            surplus = surplus - addition
    return np.array(given)


def noise(own_key, extent, spread, limit, pieces=(), kind=jnp.bfloat16):
    level = level_of(own_key, extent, pieces, -0.22, 0.18) if pieces else 1.0
    entries = jax.random.normal(own_key, extent, jnp.float32) * spread * level
    return jnp.minimum(jnp.maximum(entries, -limit), limit).astype(kind)


def setup_inputs(seed: int = 0) -> dict:
    streams_of = jax.random.split(jax.random.key(seed), 10)
    leading_batch_features = draw_leading_batch_features(jax.random.fold_in(streams_of[9], 71), 0)
    sampling_heat_selector = place_ends(jax.random.randint(streams_of[1], (LEAD_BATCH_SIZE,), 0, 4), jax.random.fold_in(streams_of[1], 1), 0, 3).astype(jnp.int32)
    output_embedding_matrix = draw_output_embedding_matrix(jax.random.fold_in(streams_of[9], 71), 0)
    trailing_batch_features = noise(streams_of[3], (TB, EMBED_DIMENSION), 1.0, 6.0, ((0, 16),))
    routed_specialist_choice_keys = jax.random.split(jax.random.fold_in(streams_of[4], 1), TB // TB_DEV)
    routed_specialist_choice_turns = jax.random.permutation(jax.random.fold_in(streams_of[4], 3), TB // TB_DEV)
    routed_specialist_choice = jax.vmap(lambda own, number: deal_out(jax.random.fold_in(streams_of[4], 2), own, number, TB_DEV, EXPERTS, TOPK, CAP, 2))(routed_specialist_choice_keys, routed_specialist_choice_turns).reshape((TB, TOPK))
    dispatcher_projection = draw_dispatcher_projection(jax.random.fold_in(streams_of[9], 71), 0)
    specialist_gating_matrix = noise(streams_of[6], (EXPERTS, EMBED_DIMENSION, FF), EMBED_DIMENSION ** -0.5, 0.109375, ((0, 16), (2, 8)))
    specialist_raising_matrix = noise(streams_of[7], (EXPERTS, EMBED_DIMENSION, FF), EMBED_DIMENSION ** -0.5, 0.109375, ((0, 16), (2, 8)))
    expert_lowering_matrix = noise(streams_of[8], (EXPERTS, FF, EMBED_DIMENSION), FF ** -0.5, 0.15625, ((0, 16), (1, 8)))
    return dict(leading_batch_features=leading_batch_features, sampling_heat_selector=sampling_heat_selector, output_embedding_matrix=output_embedding_matrix, trailing_batch_features=trailing_batch_features, routed_specialist_choice=routed_specialist_choice, dispatcher_projection=dispatcher_projection, specialist_gating_matrix=specialist_gating_matrix, specialist_raising_matrix=specialist_raising_matrix, expert_lowering_matrix=expert_lowering_matrix)


def slot_numbers(flat_ids, expert_count):
    one_hot = (flat_ids[:, None] == jnp.arange(expert_count, dtype=jnp.int32)[None, :]).astype(jnp.int32)
    earlier = jnp.cumsum(one_hot, axis=0) - one_hot
    return jnp.sum(earlier * one_hot, axis=1).astype(jnp.int32)


def reference(leading_batch_features, sampling_heat_selector, output_embedding_matrix, trailing_batch_features, routed_specialist_choice, dispatcher_projection, specialist_gating_matrix, specialist_raising_matrix, expert_lowering_matrix):
    lexicon_piece_number = math.gcd(LEAD_BATCH_SIZE, 64)
    position_heat_factor = 0.5 + 0.25 * sampling_heat_selector.astype(jnp.float32)

    def lexicon_score_piece(operands):
        token_rows, row_temps = operands
        plain_lexicon_scores = lax.dot_general(token_rows, output_embedding_matrix, (((1,), (1,)), ((), ())), preferred_element_type=jnp.float32)
        heat_divided_scores = plain_lexicon_scores / row_temps[:, None]
        row_max = jnp.max(heat_divided_scores, axis=1)
        row_total = jnp.sum(jnp.exp(heat_divided_scores - row_max[:, None]), axis=1)
        return heat_divided_scores - row_max[:, None] - jnp.log(row_total)[:, None]

    lexicon_log_probability = lax.map(lexicon_score_piece, (leading_batch_features.reshape(LEAD_BATCH_SIZE // lexicon_piece_number, lexicon_piece_number, EMBED_DIMENSION), position_heat_factor.reshape(LEAD_BATCH_SIZE // lexicon_piece_number, lexicon_piece_number)))
    lexicon_log_probability = lexicon_log_probability.reshape(LEAD_BATCH_SIZE, VOCAB)

    router_full = jnp.dot(trailing_batch_features, dispatcher_projection, preferred_element_type=jnp.float32)
    scores = jnp.take_along_axis(router_full, routed_specialist_choice, axis=1)
    gate_probs = jax.nn.softmax(scores, axis=1)
    slots = jax.vmap(lambda ids_block: slot_numbers(ids_block, EXPERTS))(routed_specialist_choice.reshape(N_EXPERT, TB_DEV * TOPK))
    slots = slots.reshape(TB, TOPK)
    block_index = (jnp.arange(TB, dtype=jnp.int32) // TB_DEV).astype(jnp.int32)
    slot_index = (routed_specialist_choice * (N_EXPERT * CAP) + block_index[:, None] * CAP + slots).reshape(-1).astype(jnp.int32)
    token_rows = jnp.repeat(trailing_batch_features, TOPK, axis=0)
    buffer = jnp.zeros((EXPERTS * N_EXPERT * CAP, EMBED_DIMENSION), jnp.bfloat16).at[slot_index].set(token_rows)
    buffer = buffer.reshape(EXPERTS, N_EXPERT * CAP, EMBED_DIMENSION)

    def one_expert(operands):
        expert_rows, w_gate, w_up, w_down = operands
        gate_proj = jnp.dot(expert_rows, w_gate, preferred_element_type=jnp.float32)
        up_proj = jnp.dot(expert_rows, w_up, preferred_element_type=jnp.float32)
        activated = (gate_proj * jax.nn.sigmoid(1.702 * gate_proj) * (up_proj + 1.0)).astype(jnp.bfloat16)
        return jnp.dot(activated, w_down, preferred_element_type=jnp.float32).astype(jnp.bfloat16)

    expert_outs = lax.map(one_expert, (buffer, specialist_gating_matrix, specialist_raising_matrix, expert_lowering_matrix))
    expert_outs = expert_outs.reshape(EXPERTS * N_EXPERT * CAP, EMBED_DIMENSION)
    picked = expert_outs[slot_index].reshape(TB, TOPK, EMBED_DIMENSION).astype(jnp.float32)
    moe_out = jnp.sum(gate_probs[:, :, None] * picked, axis=1).astype(jnp.bfloat16)
    return lexicon_log_probability, moe_out
```

```python
import functools

import jax
import jax.numpy as jnp
from jax import lax
from jax.experimental import pallas as pl
from jax.experimental.pallas import tpu as pltpu
from jax.sharding import Mesh
from jax.sharding import PartitionSpec as P

AXES = ("x", "c", "y", "z")
EXPERT = ("y", "z")
VOCAB = ("x", "c")
MESH = pl.DeviceIdType.MESH
COLS = ((0, 1024), (1024, 1024), (2048, 832))
ORDERS = (("z", "y", "x"), ("x", "z", "y"), ("y", "x", "z"))
EX, HOLD, SLOTS = 64, 4, 8


def ring(me, axis, step):
    return {axis: lax.rem(me[axis] + step, 4)}


def greet():
    me = {a: lax.axis_index(a) for a in AXES}
    barrier = pltpu.get_barrier_semaphore()
    for a in ("x", "y", "z"):
        for k in range(1, 4):
            pl.semaphore_signal(barrier, inc=1, device_id=ring(me, a, k), device_id_type=MESH)
    pl.semaphore_signal(barrier, inc=1, device_id={"c": 1 - me["c"]}, device_id_type=MESH)
    pl.semaphore_wait(barrier, 10)
    return me


def view(g, me, ranges, cols, at={}):
    idx = [ranges.get(a, at.get(a, me[a])) for a in AXES]
    return g.at[idx[0], idx[1], idx[2], idx[3], :, pl.ds(*cols)]


def remote(src, dst, ssem, rsem, dev, sends):
    cp = pltpu.make_async_remote_copy(
        src_ref=src, dst_ref=dst, send_sem=ssem, recv_sem=rsem, device_id=dev, device_id_type=MESH
    )
    cp.start()
    sends.append(cp)
    return cp


ALL = pl.ds(0, 4)


class Gather:
    def __init__(self, a, g, me, ssem, rsem, own):
        self.a, self.g, self.me, self.ssem, self.rsem = a, g, me, ssem, rsem
        self.sends, self.mates, self.got = [], [], [None] * 3
        self.own = pltpu.make_async_copy(a, g.at[me["x"], me["c"], me["y"], me["z"]], own)
        self.own.start()

    def send(self, p, k, src, dst, dev):
        return remote(src, dst, self.ssem.at[p, k], self.rsem.at[p, k], dev, self.sends)

    def first(self):
        for p in range(3):
            d = ORDERS[p][0]
            dst = view(self.g, self.me, {}, COLS[p])
            src = self.a.at[:, pl.ds(*COLS[p])]
            self.got[p] = [self.send(p, k - 1, src, dst, ring(self.me, d, k)) for k in (1, 3, 2)]

    def second(self):
        self.own.wait()
        for p in range(3):
            for cp in self.got[p]:
                cp.wait_recv()
            d0, d1, _ = ORDERS[p]
            blk = view(self.g, self.me, {d0: ALL}, COLS[p])
            self.got[p] = [self.send(p, 2 + k, blk, blk, ring(self.me, d1, k)) for k in (1, 3, 2)]

    def mate(self, p, k, blk):
        self.mates.append(self.send(p, k, blk, blk, {"c": 1 - self.me["c"]}))

    def third(self):
        for p in range(3):
            for cp in self.got[p]:
                cp.wait_recv()
            d0, d1, d2 = ORDERS[p]
            halves = [view(self.g, self.me, {d0: pl.ds(2 * h, 2), d1: ALL}, COLS[p]) for h in range(2)]
            self.got[p] = {}
            for o in range(2):
                for k, h in ((1, o), (3, 1 - o)):
                    self.got[p][k, h] = self.send(p, 6 + 2 * (k // 2) + h, halves[h], halves[h], ring(self.me, d2, k))
            blk = view(self.g, self.me, {d0: ALL, d1: ALL}, COLS[p])
            self.mate(p, 10, blk)

    def forward(self):
        self.over = [None] * 3
        for p in range(3):
            d0, d1, d2 = ORDERS[p]
            self.over[p] = []
            for k, h in ((1, 0), (3, 1)):
                self.got[p][k, h].wait_recv()
                at = ring(self.me, d2, 4 - k)
                half = view(self.g, self.me, {d0: pl.ds(2 * h, 2), d1: ALL}, COLS[p], at)
                self.over[p].append(self.send(p, 11 + h, half, half, ring(self.me, d2, k)))
        for p in range(3):
            d0, d1, d2 = ORDERS[p]
            for k, h in ((1, 0), (3, 1)):
                self.got[p][k, 1 - h].wait_recv()
                at = ring(self.me, d2, 4 - k)
                self.mate(p, 13 + h, view(self.g, self.me, {d0: ALL, d1: ALL}, COLS[p], at))

    def last(self):
        for p in range(3):
            d0, d1, d2 = ORDERS[p]
            for h in range(2):
                self.over[p][h].wait_recv()
            at = ring(self.me, d2, 2)
            self.mate(p, 15, view(self.g, self.me, {d0: ALL, d1: ALL}, COLS[p], at))

    def finish(self):
        for cp in self.mates:
            cp.wait_recv()
        for cp in self.sends:
            cp.wait_send()


def gather_kernel(t_ref, a_ref, m_ref, tg_ref, ag_ref, mg_ref, ts, tr, as_, ar, ms, mr, own):
    me = greet()
    tok = Gather(t_ref, tg_ref, me, ts, tr, own.at[0])
    tok.first()
    mine = pltpu.make_async_copy(m_ref, mg_ref.at[me["y"], me["z"]], own.at[2])
    mine.start()
    sends = []
    here = mg_ref.at[me["y"], me["z"]]
    got = [remote(m_ref, here, ms.at[k], mr.at[k], ring(me, "z", k + 1), sends) for k in range(3)]
    lead = Gather(a_ref, ag_ref, me, as_, ar, own.at[1])
    lead.first()
    tok.second()
    mine.wait()
    for cp in got:
        cp.wait_recv()
    row = mg_ref.at[me["y"]]
    got = [remote(row, row, ms.at[3 + k], mr.at[3 + k], ring(me, "y", k + 1), sends) for k in range(3)]
    tok.third()
    lead.second()
    tok.forward()
    lead.third()
    tok.last()
    lead.forward()
    tok.finish()
    for cp in got:
        cp.wait_recv()
    lead.last()
    lead.finish()
    for cp in sends:
        cp.wait_send()


def gather_all(tok, lead, meta):
    full = jax.ShapeDtypeStruct((4, 2, 4, 4) + tok.shape, tok.dtype)
    dma = pltpu.SemaphoreType.DMA
    hbm = pl.BlockSpec(memory_space=pl.ANY)
    return pl.pallas_call(
        gather_kernel,
        out_shape=(full, full, jax.ShapeDtypeStruct((4, 4, 8, 128), jnp.float32)),
        in_specs=[hbm] * 3,
        out_specs=[hbm] * 3,
        scratch_shapes=[dma((3, 16))] * 4 + [dma((6,))] * 2 + [dma((3,))],
        compiler_params=pltpu.CompilerParams(collective_id=0, has_side_effects=True),
    )(tok, lead, meta)


def join_kernel(m_ref, s_ref, o_ref, mb, sb, ssem, rsem):
    me = greet()
    mb[0, 0] = m_ref[...]
    sb[0, 0] = s_ref[...]
    sends = []
    stages = [("c", [{"c": 1 - me["c"]}])]
    stages += [(a, [ring(me, a, k) for k in range(1, 4)]) for a in ("x", "y", "z")]
    for i, (a, devs) in enumerate(stages):
        got = []
        for k, dev in enumerate(devs):
            got.append(remote(mb.at[i, 0], mb.at[i, k + 1], ssem.at[0, i, k], rsem.at[0, i, k], dev, sends))
            got.append(remote(sb.at[i, 0], sb.at[i, k + 1], ssem.at[1, i, k], rsem.at[1, i, k], dev, sends))
        for cp in got:
            cp.wait_recv()
        n = len(devs) + 1
        top = mb[i, 0]
        for k in range(1, n):
            top = jnp.maximum(top, mb[i, k])
        total = sb[i, 0] * jnp.exp(mb[i, 0] - top)
        for k in range(1, n):
            total += sb[i, k] * jnp.exp(mb[i, k] - top)
        if i < 3:
            mb[i + 1, 0] = top
            sb[i + 1, 0] = total
    o_ref[0] = top
    o_ref[1] = jnp.log(total)
    for cp in sends:
        cp.wait_send()


def joined(local_max, local_total):
    vm = pl.BlockSpec(memory_space=pltpu.VMEM)
    dma = pltpu.SemaphoreType.DMA
    out = pl.pallas_call(
        join_kernel,
        out_shape=jax.ShapeDtypeStruct((2, 8, 128), jnp.float32),
        in_specs=[vm] * 2,
        out_specs=vm,
        scratch_shapes=[pltpu.VMEM((4, 4, 8, 128), jnp.float32)] * 2 + [dma((2, 4, 3))] * 2,
        compiler_params=pltpu.CompilerParams(collective_id=1, has_side_effects=True),
    )(local_max.reshape(8, 128), local_total.reshape(8, 128))
    return out[0].reshape(-1), out[1].reshape(-1)


def routing(tok, choice, proj):
    ids = choice.T
    scores = lax.dot_general(proj, tok, (((0,), (1,)), ((), ())), preferred_element_type=jnp.float32)
    hot = (ids[:, None, :] == jnp.arange(EX, dtype=jnp.int32)[None, :, None]).astype(jnp.float32)
    picked = jnp.sum(hot * scores[None], axis=1)
    gates = jax.nn.softmax(picked, axis=0)
    n = tok.shape[0]
    before = (jnp.arange(n)[:, None] < jnp.arange(n)[None, :]).astype(jnp.float32)
    earlier = jnp.dot(jnp.sum(hot, axis=0), before, preferred_element_type=jnp.float32)
    slots = jnp.sum(hot * earlier[None], axis=1)
    keys = ids.astype(jnp.float32) * SLOTS + slots
    return jnp.pad(jnp.concatenate([keys, gates], axis=0), ((0, 0), (0, 128 - n)))


def per_device(lead, heat, embed, tok, choice, proj, w_gate, w_up, w_down):
    v = lax.axis_index(VOCAB)
    e = lax.axis_index(EXPERT)
    temp = 0.5 + 0.25 * heat.astype(jnp.float32)
    meta = routing(tok, choice, proj)
    tg, ag, mg = gather_all(lax.dynamic_slice_in_dim(tok, v * 8, 8, 0), lead, meta)
    tokens = tg.reshape(8, 16, 8, -1).transpose(1, 0, 2, 3).reshape(4, 256, -1)
    rows = ag.reshape(1024, -1)
    meta_all = mg.reshape(16, 8, 128)[:, :, :64]
    keys = meta_all[:, :4] - (e * (HOLD * SLOTS)).astype(jnp.float32)
    near = (keys >= 0) & (keys < HOLD * SLOTS)
    keys = jnp.where(near, keys + 32.0 * (jnp.arange(16) % 4)[:, None, None], -1.0)
    keys = keys.reshape(4, 4, 4, 64).transpose(0, 2, 1, 3).reshape(4, 4, 256)
    gates = meta_all[:, 4:].reshape(4, 4, 4, 64).transpose(0, 2, 1, 3).reshape(4, 4, 256)
    eq = keys[:, :, None, :] == jnp.arange(128, dtype=jnp.float32)[None, None, :, None]
    hot = jnp.sum(eq.astype(jnp.float32), axis=1)
    gate_of = jnp.sum(jnp.sum(jnp.where(eq, gates[:, :, None, :], 0.0), axis=1), axis=2)
    hot = hot.astype(jnp.bfloat16)
    picked = jnp.einsum("gst,gtd->gsd", hot, tokens, preferred_element_type=jnp.float32).astype(jnp.bfloat16)
    picked = picked.reshape(16, HOLD, SLOTS, -1)
    gp = jnp.einsum("secd,edf->secf", picked, w_gate, preferred_element_type=jnp.float32)
    up = jnp.einsum("secd,edf->secf", picked, w_up, preferred_element_type=jnp.float32)
    act = (gp * jax.nn.sigmoid(1.702 * gp) * (up + 1.0)).astype(jnp.bfloat16)
    part = jnp.einsum("secf,efd->secd", act, w_down, preferred_element_type=jnp.float32)
    part = part.reshape(4, 128, -1) * gate_of[:, :, None]
    high = part.astype(jnp.bfloat16)
    low = (part - high.astype(jnp.float32)).astype(jnp.bfloat16)
    mixed = jnp.einsum("gst,gsd->gtd", hot, high, preferred_element_type=jnp.float32)
    mixed += jnp.einsum("gst,gsd->gtd", hot, low, preferred_element_type=jnp.float32)
    mixed = mixed.reshape(1024, -1)
    mine = lax.all_to_all(mixed.astype(jnp.bfloat16).reshape(1024, 8, 360).transpose(1, 0, 2), VOCAB, 0, 0, tiled=True)
    mine = jnp.sum(mine.astype(jnp.float32), axis=0).astype(jnp.bfloat16).reshape(16, 64, 360)
    mine = lax.all_to_all(mine, EXPERT, 0, 0, tiled=True)
    moe = jnp.sum(mine.astype(jnp.float32), axis=0).astype(jnp.bfloat16)

    scaled = lax.dot_general(rows, embed, (((1,), (1,)), ((), ())), preferred_element_type=jnp.float32)
    scaled = scaled / temp[:, None]
    top = jnp.max(scaled, axis=1)
    total = jnp.sum(jnp.exp(scaled - top[:, None]), axis=1)
    top, log_total = joined(top, total)
    return scaled - top[:, None] - log_total[:, None], moe


def solution(mesh):
    torus = Mesh(mesh.devices.reshape(4, 2, 4, 4), AXES)
    placed = (
        P(AXES, None), P(), P(AXES, None), P(EXPERT, None), P(EXPERT, None), P(),
        P(EXPERT, None, VOCAB), P(EXPERT, None, VOCAB), P(EXPERT, VOCAB, None),
    )
    return jax.shard_map(
        per_device, mesh=torus, in_specs=placed,
        out_specs=(P(None, AXES), P(EXPERT, VOCAB)), check_vma=False,
    )
```

```python
import functools

import jax
import jax.numpy as jnp
from jax import lax
from jax.experimental import pallas as pl
from jax.experimental.pallas import tpu as pltpu
from jax.sharding import Mesh
from jax.sharding import PartitionSpec as P

AXES = ("x", "c", "y", "z")
EXPERT = ("y", "z")
VOCAB = ("x", "c")
MESH = pl.DeviceIdType.MESH
COLS = ((0, 1024), (1024, 1024), (2048, 832))
ORDERS = (("z", "y", "x"), ("x", "z", "y"), ("y", "x", "z"))
EX, HOLD, SLOTS = 64, 4, 8


def ring(me, axis, step):
    return {axis: lax.rem(me[axis] + step, 4)}


def greet():
    me = {a: lax.axis_index(a) for a in AXES}
    barrier = pltpu.get_barrier_semaphore()
    for a in ("x", "y", "z"):
        for k in range(1, 4):
            pl.semaphore_signal(barrier, inc=1, device_id=ring(me, a, k), device_id_type=MESH)
    pl.semaphore_signal(barrier, inc=1, device_id={"c": 1 - me["c"]}, device_id_type=MESH)
    pl.semaphore_wait(barrier, 10)
    return me


def view(g, dims, me, ranges, cols, at={}):
    idx = [ranges.get(a, at.get(a, me[a])) for a in dims]
    return g.at[idx[0], idx[1], idx[2], idx[3], :, pl.ds(*cols)]


def remote(src, dst, ssem, rsem, dev, sends):
    cp = pltpu.make_async_remote_copy(
        src_ref=src, dst_ref=dst, send_sem=ssem, recv_sem=rsem, device_id=dev, device_id_type=MESH
    )
    cp.start()
    sends.append(cp)
    return cp


ALL = pl.ds(0, 4)


class Gather:
    def __init__(self, a, g, dims, me, ssem, rsem, own):
        self.dims = dims
        self.a, self.g, self.me, self.ssem, self.rsem = a, g, me, ssem, rsem
        self.sends, self.mates, self.got = [], [], [None] * 3
        self.own = pltpu.make_async_copy(a, g.at[tuple(me[d] for d in dims)], own)
        self.own.start()

    def send(self, p, k, src, dst, dev):
        return remote(src, dst, self.ssem.at[p, k], self.rsem.at[p, k], dev, self.sends)

    def first(self):
        for p in range(3):
            d = ORDERS[p][0]
            dst = view(self.g, self.dims, self.me, {}, COLS[p])
            src = self.a.at[:, pl.ds(*COLS[p])]
            self.got[p] = [self.send(p, k - 1, src, dst, ring(self.me, d, k)) for k in (1, 3, 2)]

    def second(self):
        self.own.wait()
        for p in range(3):
            for cp in self.got[p]:
                cp.wait_recv()
            d0, d1, _ = ORDERS[p]
            blk = view(self.g, self.dims, self.me, {d0: ALL}, COLS[p])
            self.got[p] = [self.send(p, 2 + k, blk, blk, ring(self.me, d1, k)) for k in (1, 3, 2)]

    def mate(self, p, k, blk):
        self.mates.append(self.send(p, k, blk, blk, {"c": 1 - self.me["c"]}))

    def third(self):
        for p in range(3):
            for cp in self.got[p]:
                cp.wait_recv()
            d0, d1, d2 = ORDERS[p]
            halves = [view(self.g, self.dims, self.me, {d0: pl.ds(2 * h, 2), d1: ALL}, COLS[p]) for h in range(2)]
            self.got[p] = {}
            for o in range(2):
                for k, h in ((1, o), (3, 1 - o)):
                    self.got[p][k, h] = self.send(p, 6 + 2 * (k // 2) + h, halves[h], halves[h], ring(self.me, d2, k))
            blk = view(self.g, self.dims, self.me, {d0: ALL, d1: ALL}, COLS[p])
            self.mate(p, 10, blk)

    def forward(self):
        self.over = [None] * 3
        for p in range(3):
            d0, d1, d2 = ORDERS[p]
            self.over[p] = []
            for k, h in ((1, 0), (3, 1)):
                self.got[p][k, h].wait_recv()
                at = ring(self.me, d2, 4 - k)
                half = view(self.g, self.dims, self.me, {d0: pl.ds(2 * h, 2), d1: ALL}, COLS[p], at)
                self.over[p].append(self.send(p, 11 + h, half, half, ring(self.me, d2, k)))
        for p in range(3):
            d0, d1, d2 = ORDERS[p]
            for k, h in ((1, 0), (3, 1)):
                self.got[p][k, 1 - h].wait_recv()
                at = ring(self.me, d2, 4 - k)
                self.mate(p, 13 + h, view(self.g, self.dims, self.me, {d0: ALL, d1: ALL}, COLS[p], at))

    def last(self):
        for p in range(3):
            d0, d1, d2 = ORDERS[p]
            for h in range(2):
                self.over[p][h].wait_recv()
            at = ring(self.me, d2, 2)
            self.mate(p, 15, view(self.g, self.dims, self.me, {d0: ALL, d1: ALL}, COLS[p], at))

    def arrive(self):
        for cp in self.mates:
            cp.wait_recv()

    def drain(self):
        for cp in self.sends:
            cp.wait_send()


def plan(meta_row, base):
    slot = lax.broadcasted_iota(jnp.int32, (128, 256), 0).astype(jnp.float32)
    src = (lax.broadcasted_iota(jnp.int32, (1, 256), 1) // 64).astype(jnp.float32) * 32.0
    hot = jnp.zeros((128, 256), jnp.float32)
    gates = jnp.zeros((128, 256), jnp.float32)
    for k in range(4):
        key = meta_row[k : k + 1] - base
        key = jnp.where((key >= 0.0) & (key < 32.0), key + src, -1.0)
        eq = slot == key
        hot += jnp.where(eq, 1.0, 0.0)
        gates += jnp.where(eq, meta_row[4 + k : 5 + k], 0.0)
    return hot.astype(jnp.bfloat16), jnp.sum(gates, axis=1, keepdims=True)


def copy(src, dst, sem):
    cp = pltpu.make_async_copy(src, dst, sem)
    cp.start()
    return cp


def dot(a, b, ca, cb):
    return lax.dot_general(a, b, (((ca,), (cb,)), ((), ())), preferred_element_type=jnp.float32)


def a_kernel(
    t_ref, a_ref, m_ref, wg_ref, wu_ref, wd_ref,
    ag_ref, tg_ref, act_ref, mg_ref, wdp_ref,
    wg, wu, wraw, wdp, mg, tok, xs,
    ts, tr, as_, ar, ms, mr, own, rawsem, outsem, toksem,
):
    me = greet()
    tok_g = Gather(t_ref, tg_ref, ("y", "z", "x", "c"), me, ts, tr, own.at[0])
    tok_g.first()
    mine = copy(m_ref, mg.at[me["y"], me["z"]], own.at[2])
    raw = copy(wd_ref, wraw, rawsem.at[0])
    sends = []
    here = mg.at[me["y"], me["z"]]
    mgot = [remote(m_ref, here, ms.at[k], mr.at[k], ring(me, "z", k + 1), sends) for k in range(3)]
    lead = Gather(a_ref, ag_ref, AXES, me, as_, ar, own.at[1])
    lead.first()
    raw.wait()
    tok_g.second()

    def low(i, _):
        r = wraw[pl.ds(i * 4, 4)].reshape(16, 2880)
        for v in range(8):
            rows = pl.ds(pl.multiple_of(i * 16, 16), 16)
            wdp[v % 2, rows, pl.ds((v // 2) * 384, 360)] = r[:, 360 * v : 360 * v + 360]
            wdp[v % 2, rows, pl.ds((v // 2) * 384 + 360, 24)] = jnp.zeros((16, 24), jnp.bfloat16)
        return 0

    lax.fori_loop(0, 45, low, 0)
    low_out = copy(wdp, wdp_ref, outsem.at[0])
    mine.wait()
    for cp in mgot:
        cp.wait_recv()
    row = mg.at[me["y"]]
    mgot = [remote(row, row, ms.at[3 + k], mr.at[3 + k], ring(me, "y", k + 1), sends) for k in range(3)]
    raw = copy(wg_ref, wraw, rawsem.at[1])
    tok_g.third()
    lead.second()
    raw.wait()

    def flat(dst):
        def body(i, _):
            dst[pl.ds(pl.multiple_of(i * 16, 16), 16), :] = wraw[pl.ds(i * 4, 4)].reshape(16, 2880)
            return 0

        lax.fori_loop(0, 45, body, 0)

    flat(wg)
    raw = copy(wu_ref, wraw, rawsem.at[2])
    tok_g.forward()
    lead.third()
    raw.wait()
    flat(wu)
    tok_g.last()
    tok_g.arrive()
    for cp in mgot:
        cp.wait_recv()
    mg_out = copy(mg, mg_ref, outsem.at[1])
    base = ((me["y"] * 4 + me["z"]) * 32).astype(jnp.float32)
    flat_tok = tg_ref.reshape(1024, 2880)
    loads = [copy(flat_tok.at[pl.ds(0, 256)], tok.at[0], toksem.at[0])]
    for g in range(4):
        if g < 3:
            loads.append(copy(flat_tok.at[pl.ds(256 * (g + 1), 256)], tok.at[(g + 1) % 2], toksem.at[g + 1]))
        loads[g].wait()
        row = jnp.concatenate([mg[g, 0] + mg[g, 1], mg[g, 2] + mg[g, 3]], axis=1)
        hot, _ = plan(row, base)
        xs[pl.ds(128 * g, 128), :] = dot(hot, tok[g % 2], 1, 0).astype(jnp.bfloat16)
    lead.forward()

    def ffn(i, _):
        rows = pl.ds(pl.multiple_of(i * 128, 128), 128)
        x = xs[rows, :]
        gp = dot(x, wg[...], 1, 1)
        up = dot(x, wu[...], 1, 1)
        r = lax.broadcasted_iota(jnp.int32, (128, 720), 0)
        c = lax.broadcasted_iota(jnp.int32, (128, 720), 1)
        keep = lax.rem(lax.div(r, 8), 4) == lax.rem(c, 4)
        h = gp * jax.nn.sigmoid(1.702 * gp) * (up + 1.0)
        act_ref[rows, :] = jnp.where(keep, h, 0.0).astype(jnp.bfloat16)
        return 0

    lax.fori_loop(0, 4, ffn, 0)
    lead.last()
    lead.arrive()
    low_out.wait()
    mg_out.wait()
    tok_g.drain()
    lead.drain()
    for cp in sends:
        cp.wait_send()


def kernel_a(tok, lead, meta, w_gate, w_up, w_down):
    bf = jnp.bfloat16
    full = jax.ShapeDtypeStruct((4, 2, 4, 4, 8, 2880), bf)
    tfull = jax.ShapeDtypeStruct((4, 4, 4, 2, 8, 2880), bf)
    dma = pltpu.SemaphoreType.DMA
    hbm = pl.BlockSpec(memory_space=pl.ANY)
    vm = pl.BlockSpec(memory_space=pltpu.VMEM)
    return pl.pallas_call(
        a_kernel,
        out_shape=(
            full, tfull, jax.ShapeDtypeStruct((512, 720), bf),
            jax.ShapeDtypeStruct((4, 4, 8, 128), jnp.float32), jax.ShapeDtypeStruct((2, 720, 1536), bf),
        ),
        in_specs=[hbm] * 6,
        out_specs=[hbm, hbm, vm, hbm, hbm],
        scratch_shapes=[
            pltpu.VMEM((720, 2880), bf), pltpu.VMEM((720, 2880), bf), pltpu.VMEM((180, 4, 2880), bf),
            pltpu.VMEM((2, 720, 1536), bf), pltpu.VMEM((4, 4, 8, 128), jnp.float32),
            pltpu.VMEM((2, 256, 2880), bf), pltpu.VMEM((512, 2880), bf),
        ]
        + [dma((3, 16))] * 4 + [dma((6,))] * 2 + [dma((3,)), dma((3,)), dma((2,)), dma((4,))],
        compiler_params=pltpu.CompilerParams(collective_id=0, has_side_effects=True, vmem_limit_bytes=60 * 2**20),
    )(tok, lead, meta, w_gate, w_up, w_down)


BACK = (("z", "y", "x"), ("x", "z", "y"), ("y", "x", "z"))
DEST = ("x", "y", "z")
VB, NV, VOC = 392, 4, 1571


def b_kernel(
    act_ref, m_ref, it_ref, wdp_ref, emb_ref, ag_ref,
    sc_ref, st_ref, moe_ref,
    wd, emb, rows, lg, to_mate, from_mate, own, out1, in1, sum1, out2, in2, sum2, out3, in3, mb, sb,
    wsem, esem, xsem, lsem, hs, hr, s1, r1, s2, r2, s3, r3, ssem, rsem,
):
    c = lax.axis_index("c")
    wload = [copy(wdp_ref.at[1 - c], wd.at[0], wsem.at[0]), copy(wdp_ref.at[c], wd.at[1], wsem.at[1])]
    eload = copy(emb_ref, emb, esem)
    flat = ag_ref.reshape(1024, 2880)
    xload = [copy(flat.at[pl.ds(256 * i, 256)], rows.at[i], xsem.at[i]) for i in range(2)]
    me = greet()
    sends = []
    base = ((me["y"] * 4 + me["z"]) * 32).astype(jnp.float32)
    mate = {"c": 1 - me["c"]}
    hgot = []
    for half in range(2):
        wload[half].wait()
        for g in range(4):
            row = jnp.concatenate([m_ref[g, 0] + m_ref[g, 1], m_ref[g, 2] + m_ref[g, 3]], axis=1)
            hot, gate = plan(row, base)
            y = dot(act_ref[pl.ds(128 * g, 128), :], wd[half], 1, 0) * gate
            high = y.astype(jnp.bfloat16)
            low = (y - high.astype(jnp.float32)).astype(jnp.bfloat16)
            mix = dot(jnp.concatenate([hot, hot], axis=0), jnp.concatenate([high, low], axis=0), 0, 0)
            for x in range(4):
                for p in range(3):
                    piece = mix[:, 384 * x + 128 * p : 384 * x + 128 * (p + 1)].reshape(4, 64, 128)
                    if half == 0:
                        to_mate[p, x, g] = piece.astype(jnp.bfloat16)
                    else:
                        own[p, x, g] = piece
            if half == 0:
                hgot.append(remote(to_mate.at[:, :, g], from_mate.at[:, :, g], hs.at[g], hr.at[g], mate, sends))
    for cp in hgot:
        cp.wait_recv()

    def index(p, at, full):
        return (p,) + tuple(at[d] if d in at else pl.ds(0, 4) for d in full)

    got1 = []
    for p in range(3):
        d = BACK[p][0]
        rest = [a for a in DEST if a != d]
        for k in (1, 3, 2):
            i = index(p, ring(me, d, k), DEST)
            out1[p, k - 1] = (own[i] + from_mate[i].astype(jnp.float32)).astype(jnp.bfloat16)
            got1.append((p, k, remote(out1.at[p, k - 1], in1.at[p, k - 1], s1.at[p, k - 1], r1.at[p, k - 1], ring(me, d, k), sends)))
        i = index(p, {d: me[d]}, DEST)
        sum1[p] = own[i] + from_mate[i].astype(jnp.float32)

    eload.wait()
    stores = []
    for j in range(4):
        xload[j].wait()
        inv = it_ref[:, pl.ds(256 * j, 256)]
        if j >= 2:
            stores[j - 2].wait()
        buf = lg.at[j % 2]

        def block(i0, n, top):
            r = dot(emb[pl.ds(i0, n), :], rows[j % 2], 1, 1) * inv
            buf[pl.ds(i0, n), :] = r
            return jnp.maximum(top, jnp.max(r, axis=0, keepdims=True))

        top = jnp.full((1, 256), -jnp.inf, jnp.float32)
        top = lax.fori_loop(0, NV, lambda i, t: block(pl.multiple_of(i * VB, 8), VB, t), top)
        top = block(NV * VB, VOC - NV * VB, top)
        if j < 2:
            xload.append(copy(flat.at[pl.ds(256 * (j + 2), 256)], rows.at[j], xsem.at[j + 2]))

        def tail(i, s):
            return s + jnp.sum(jnp.exp(buf[pl.ds(pl.multiple_of(i * 112, 8), 112), :] - top), axis=0, keepdims=True)

        total = lax.fori_loop(0, 14, tail, jnp.zeros((1, 256), jnp.float32))
        total += jnp.sum(jnp.exp(buf[pl.ds(1568, 3), :] - top), axis=0, keepdims=True)
        for h in range(2):
            mb[0, 0, pl.ds(2 * j + h, 1), :] = top[:, 128 * h : 128 * (h + 1)]
            sb[0, 0, pl.ds(2 * j + h, 1), :] = total[:, 128 * h : 128 * (h + 1)]
        stores.append(copy(buf, sc_ref.at[:, pl.ds(256 * j, 256)], lsem.at[j]))

    stages = [[mate]] + [[ring(me, a, k) for k in range(1, 4)] for a in DEST]

    def begin(i):
        got = []
        for k, dev in enumerate(stages[i]):
            got.append(remote(mb.at[i, 0], mb.at[i, k + 1], ssem.at[0, i, k], rsem.at[0, i, k], dev, sends))
            got.append(remote(sb.at[i, 0], sb.at[i, k + 1], ssem.at[1, i, k], rsem.at[1, i, k], dev, sends))
        return got

    def end(i, got):
        for cp in got:
            cp.wait_recv()
        n = len(stages[i]) + 1
        top = mb[i, 0]
        for k in range(1, n):
            top = jnp.maximum(top, mb[i, k])
        total = sb[i, 0] * jnp.exp(mb[i, 0] - top)
        for k in range(1, n):
            total += sb[i, k] * jnp.exp(mb[i, k] - top)
        if i < 3:
            mb[i + 1, 0] = top
            sb[i + 1, 0] = total
        else:
            st_ref[...] = top + jnp.log(total)

    got = begin(0)
    for p, k, cp in got1:
        cp.wait_recv()
        sum1[p] += in1[p, k - 1].astype(jnp.float32)
    got2 = []
    for p in range(3):
        _, d, e = BACK[p]
        first = [a for a in DEST if a != BACK[p][0]]
        for k in (1, 3, 2):
            i = index(p, ring(me, d, k), first)
            out2[p, k - 1] = sum1[i].astype(jnp.bfloat16)
            got2.append((p, k, remote(out2.at[p, k - 1], in2.at[p, k - 1], s2.at[p, k - 1], r2.at[p, k - 1], ring(me, d, k), sends)))
        sum2[p] = sum1[index(p, {d: me[d]}, first)]
    end(0, got)
    got = begin(1)
    for p, k, cp in got2:
        cp.wait_recv()
        sum2[p] += in2[p, k - 1].astype(jnp.float32)
    got3 = []
    for p in range(3):
        d = BACK[p][2]
        for k in (1, 3, 2):
            out3[p, k - 1] = sum2[p, lax.rem(me[d] + k, 4)]
            got3.append((p, k, remote(out3.at[p, k - 1], in3.at[p, k - 1], s3.at[p, k - 1], r3.at[p, k - 1], ring(me, d, k), sends)))
    end(1, got)
    got = begin(2)
    for p, k, cp in got3:
        cp.wait_recv()
    for p in range(3):
        total = sum2[p, me[BACK[p][2]]]
        for k in range(3):
            total += in3[p, k]
        n = 128 if p < 2 else 104
        moe_ref[:, pl.ds(128 * p, n)] = total[:, :n].astype(jnp.bfloat16)
    end(2, got)
    got = begin(3)
    stores[2].wait()
    stores[3].wait()
    end(3, got)
    for cp in sends:
        cp.wait_send()


def kernel_b(act, meta, inv_temp, wdp, embed, lead):
    bf, f32 = jnp.bfloat16, jnp.float32
    dma = pltpu.SemaphoreType.DMA
    hbm = pl.BlockSpec(memory_space=pl.ANY)
    vm = pl.BlockSpec(memory_space=pltpu.VMEM)
    V = pltpu.VMEM
    return pl.pallas_call(
        b_kernel,
        out_shape=(
            jax.ShapeDtypeStruct((VOC, 1024), f32), jax.ShapeDtypeStruct((8, 128), f32),
            jax.ShapeDtypeStruct((64, 360), bf),
        ),
        in_specs=[vm, vm, vm, hbm, hbm, hbm],
        out_specs=[hbm, vm, vm],
        scratch_shapes=[
            V((2, 720, 1536), bf), V((VOC, 2880), bf), V((2, 256, 2880), bf), V((2, VOC, 256), f32),
            V((3, 4, 4, 4, 64, 128), bf), V((3, 4, 4, 4, 64, 128), bf), V((3, 4, 4, 4, 64, 128), f32),
            V((3, 3, 4, 4, 64, 128), bf), V((3, 3, 4, 4, 64, 128), bf), V((3, 4, 4, 64, 128), f32),
            V((3, 3, 4, 64, 128), bf), V((3, 3, 4, 64, 128), bf), V((3, 4, 64, 128), f32),
            V((3, 3, 64, 128), f32), V((3, 3, 64, 128), f32),
            V((4, 4, 8, 128), f32), V((4, 4, 8, 128), f32),
            dma((2,)), dma, dma((4,)), dma((4,)), dma((4,)), dma((4,)),
        ]
        + [dma((3, 3))] * 6 + [dma((2, 4, 3))] * 2,
        compiler_params=pltpu.CompilerParams(collective_id=1, has_side_effects=True, vmem_limit_bytes=63 * 2**20),
    )(act, meta, inv_temp, wdp, embed, lead)


def c_kernel(s_ref, t_ref, o_ref):
    o_ref[...] = s_ref[...] - t_ref[...]


def kernel_c(scaled, shift):
    n = 200
    blk = pl.BlockSpec((n, 1024), lambda i: (i, 0))
    return pl.pallas_call(
        c_kernel, grid=(pl.cdiv(VOC, n),), out_shape=jax.ShapeDtypeStruct((VOC, 1024), jnp.float32),
        in_specs=[blk, pl.BlockSpec((1, 1024), lambda i: (0, 0))], out_specs=blk,
    )(scaled, shift)


def routing(tok, choice, proj):
    ids = choice.T
    scores = lax.dot_general(proj, tok, (((0,), (1,)), ((), ())), preferred_element_type=jnp.float32)
    hot = (ids[:, None, :] == jnp.arange(EX, dtype=jnp.int32)[None, :, None]).astype(jnp.float32)
    picked = jnp.sum(hot * scores[None], axis=1)
    gates = jax.nn.softmax(picked, axis=0)
    n = tok.shape[0]
    before = (jnp.arange(n)[:, None] < jnp.arange(n)[None, :]).astype(jnp.float32)
    earlier = jnp.dot(jnp.sum(hot, axis=0), before, preferred_element_type=jnp.float32)
    slots = jnp.sum(hot * earlier[None], axis=1)
    keys = ids.astype(jnp.float32) * SLOTS + slots
    both = jnp.concatenate([keys, gates], axis=0)
    odd = lax.axis_index("z") % 2 == 1
    zero = jnp.zeros_like(both)
    return jnp.concatenate([jnp.where(odd, zero, both), jnp.where(odd, both, zero)], axis=1)


def per_device(lead, heat, embed, tok, choice, proj, w_gate, w_up, w_down):
    v = lax.axis_index(VOCAB)
    inv_temp = (1.0 / (0.5 + 0.25 * heat.astype(jnp.float32))).reshape(1, 1024)
    meta = routing(tok, choice, proj)
    flip = lambda w: jnp.transpose(w, (2, 0, 1))
    mine = lax.dynamic_slice_in_dim(tok, v * 8, 8, 0)
    rows, _, act, keys, wdp = kernel_a(
        mine, lead, meta, flip(w_gate), flip(w_up), jnp.transpose(w_down, (1, 0, 2))
    )
    scaled, shift, moe = kernel_b(act, keys, inv_temp, wdp, embed, rows)
    return kernel_c(scaled, shift.reshape(1, 1024)).T, moe


def solution(mesh):
    torus = Mesh(mesh.devices.reshape(4, 2, 4, 4), AXES)
    placed = (
        P(AXES, None), P(), P(AXES, None), P(EXPERT, None), P(EXPERT, None), P(),
        P(EXPERT, None, VOCAB), P(EXPERT, None, VOCAB), P(EXPERT, VOCAB, None),
    )
    return jax.shard_map(
        per_device, mesh=torus, in_specs=placed,
        out_specs=(P(None, AXES), P(EXPERT, VOCAB)), check_vma=False,
    )
```

```python
import functools

import jax
import jax.numpy as jnp
from jax import lax
from jax.experimental import pallas as pl
from jax.experimental.pallas import tpu as pltpu
from jax.sharding import Mesh
from jax.sharding import PartitionSpec as P

AXES = ("x", "c", "y", "z")
EXPERT = ("y", "z")
VOCAB = ("x", "c")
MESH = pl.DeviceIdType.MESH
COLS = ((0, 1024), (1024, 1024), (2048, 832))
ORDERS = (("z", "y", "x"), ("x", "z", "y"), ("y", "x", "z"))
EX, HOLD, SLOTS = 64, 4, 8


def ring(me, axis, step):
    return {axis: lax.rem(me[axis] + step, 4)}


def greet():
    me = {a: lax.axis_index(a) for a in AXES}
    barrier = pltpu.get_barrier_semaphore()
    for a in ("x", "y", "z"):
        for k in range(1, 4):
            pl.semaphore_signal(barrier, inc=1, device_id=ring(me, a, k), device_id_type=MESH)
    pl.semaphore_signal(barrier, inc=1, device_id={"c": 1 - me["c"]}, device_id_type=MESH)
    pl.semaphore_wait(barrier, 10)
    return me


def view(g, dims, me, ranges, cols, at={}):
    idx = [ranges.get(a, at.get(a, me[a])) for a in dims]
    return g.at[idx[0], idx[1], idx[2], idx[3], :, pl.ds(*cols)]


def remote(src, dst, ssem, rsem, dev, sends):
    cp = pltpu.make_async_remote_copy(
        src_ref=src, dst_ref=dst, send_sem=ssem, recv_sem=rsem, device_id=dev, device_id_type=MESH
    )
    cp.start()
    sends.append(cp)
    return cp


ALL = pl.ds(0, 4)


class Gather:
    def __init__(self, a, g, dims, me, ssem, rsem, own):
        self.dims = dims
        self.a, self.g, self.me, self.ssem, self.rsem = a, g, me, ssem, rsem
        self.sends, self.mates, self.got = [], [], [None] * 3
        self.own = pltpu.make_async_copy(a, g.at[tuple(me[d] for d in dims)], own)
        self.own.start()

    def send(self, p, k, src, dst, dev):
        return remote(src, dst, self.ssem.at[p, k], self.rsem.at[p, k], dev, self.sends)

    def first(self):
        for p in range(3):
            d = ORDERS[p][0]
            dst = view(self.g, self.dims, self.me, {}, COLS[p])
            src = self.a.at[:, pl.ds(*COLS[p])]
            self.got[p] = [self.send(p, k - 1, src, dst, ring(self.me, d, k)) for k in (1, 3, 2)]

    def second(self):
        self.own.wait()
        for p in range(3):
            for cp in self.got[p]:
                cp.wait_recv()
            d0, d1, _ = ORDERS[p]
            blk = view(self.g, self.dims, self.me, {d0: ALL}, COLS[p])
            self.got[p] = [self.send(p, 2 + k, blk, blk, ring(self.me, d1, k)) for k in (1, 3, 2)]

    def mate(self, p, k, blk):
        self.mates.append(self.send(p, k, blk, blk, {"c": 1 - self.me["c"]}))

    def third(self):
        for p in range(3):
            for cp in self.got[p]:
                cp.wait_recv()
            d0, d1, d2 = ORDERS[p]
            halves = [view(self.g, self.dims, self.me, {d0: pl.ds(2 * h, 2), d1: ALL}, COLS[p]) for h in range(2)]
            self.got[p] = {}
            for o in range(2):
                for k, h in ((1, o), (3, 1 - o)):
                    self.got[p][k, h] = self.send(p, 6 + 2 * (k // 2) + h, halves[h], halves[h], ring(self.me, d2, k))
            blk = view(self.g, self.dims, self.me, {d0: ALL, d1: ALL}, COLS[p])
            self.mate(p, 10, blk)

    def forward(self):
        self.over = [None] * 3
        for p in range(3):
            d0, d1, d2 = ORDERS[p]
            self.over[p] = []
            for k, h in ((1, 0), (3, 1)):
                self.got[p][k, h].wait_recv()
                at = ring(self.me, d2, 4 - k)
                half = view(self.g, self.dims, self.me, {d0: pl.ds(2 * h, 2), d1: ALL}, COLS[p], at)
                self.over[p].append(self.send(p, 11 + h, half, half, ring(self.me, d2, k)))
        for p in range(3):
            d0, d1, d2 = ORDERS[p]
            for k, h in ((1, 0), (3, 1)):
                self.got[p][k, 1 - h].wait_recv()
                at = ring(self.me, d2, 4 - k)
                self.mate(p, 13 + h, view(self.g, self.dims, self.me, {d0: ALL, d1: ALL}, COLS[p], at))

    def last(self):
        for p in range(3):
            d0, d1, d2 = ORDERS[p]
            for h in range(2):
                self.over[p][h].wait_recv()
            at = ring(self.me, d2, 2)
            self.mate(p, 15, view(self.g, self.dims, self.me, {d0: ALL, d1: ALL}, COLS[p], at))

    def arrive(self):
        for cp in self.mates:
            cp.wait_recv()

    def drain(self):
        for cp in self.sends:
            cp.wait_send()


def plan(meta_row, base):
    slot = lax.broadcasted_iota(jnp.int32, (128, 256), 0).astype(jnp.float32)
    src = (lax.broadcasted_iota(jnp.int32, (1, 256), 1) // 64).astype(jnp.float32) * 32.0
    hot = jnp.zeros((128, 256), jnp.float32)
    gates = jnp.zeros((128, 256), jnp.float32)
    for k in range(4):
        key = meta_row[k : k + 1] - base
        key = jnp.where((key >= 0.0) & (key < 32.0), key + src, -1.0)
        eq = slot == key
        hot += jnp.where(eq, 1.0, 0.0)
        gates += jnp.where(eq, meta_row[4 + k : 5 + k], 0.0)
    return hot.astype(jnp.bfloat16), jnp.sum(gates, axis=1, keepdims=True)


def copy(src, dst, sem):
    cp = pltpu.make_async_copy(src, dst, sem)
    cp.start()
    return cp


def dot(a, b, ca, cb):
    return lax.dot_general(a, b, (((ca,), (cb,)), ((), ())), preferred_element_type=jnp.float32)


BACK = (("z", "y", "x"), ("x", "z", "y"), ("y", "x", "z"))
DEST = ("x", "y", "z")
VOC = 1571
BLOCKS = ((0, 528), (528, 528), (1056, 515))


def routing(ids, proj, tok, odd):
    scores = dot(proj, tok, 1, 1)
    expert = lax.broadcasted_iota(jnp.int32, (EX, 128), 0)
    hot = [(expert == ids[k : k + 1]).astype(jnp.float32) for k in range(4)]
    picked = [jnp.sum(h * scores, axis=0, keepdims=True) for h in hot]
    top = jnp.maximum(jnp.maximum(picked[0], picked[1]), jnp.maximum(picked[2], picked[3]))
    weights = [jnp.exp(p - top) for p in picked]
    total = weights[0] + weights[1] + weights[2] + weights[3]
    a = lax.broadcasted_iota(jnp.int32, (128, 128), 0)
    b = lax.broadcasted_iota(jnp.int32, (128, 128), 1)
    before = ((a < 64) & (a < lax.rem(b, 64))).astype(jnp.bfloat16)
    named = hot[0] + hot[1] + hot[2] + hot[3]
    earlier = dot(named.astype(jnp.bfloat16), before, 1, 0)
    lane = lax.broadcasted_iota(jnp.int32, (1, 128), 1)
    here = lax.div(lane, 64) == odd
    rows = []
    for k in range(4):
        slot = jnp.sum(hot[k] * earlier, axis=0, keepdims=True)
        rows.append(jnp.where(here, ids[k : k + 1].astype(jnp.float32) * SLOTS + slot, 0.0))
    for k in range(4):
        rows.append(jnp.where(here, weights[k] / total, 0.0))
    return rows


def main_kernel(
    t_ref, a_ref, id_ref, pj_ref, heat_ref, wg_ref, wu_ref, wd_ref, emb_ref,
    sc_ref, st_ref, moe_ref, ag_ref, tg_ref,
    wg, wu, wraw, wd, mine, mg, rows, xs, act, hots, gates, tok2,
    emb, lg, to_mate, from_mate, own, in1, sum1, out2, in2, sum2, out3, in3, mb, sb,
    ts, tr, as_, ar, ms, mr, loc, rawsem, toksem, esem, xsem, lsem,
    hs, hr, s1, r1, s2, r2, s3, r3, ssem, rsem,
):
    c = lax.axis_index("c")
    load = [copy(t_ref, tok2.at[pl.ds(64 * h, 64)], loc.at[2 + h]) for h in range(2)]
    me = greet()
    sends = []
    v = me["x"] * 2 + me["c"]
    mate = {"c": 1 - me["c"]}
    tok = Gather(t_ref.at[pl.ds(pl.multiple_of(v * 8, 8), 8)], tg_ref, ("y", "z", "x", "c"), me, ts, tr, loc.at[0])
    tok.first()
    lead = Gather(a_ref, ag_ref, AXES, me, as_, ar, loc.at[1])
    lead.first()
    raw = copy(wd_ref, wraw, rawsem.at[0])
    for cp in load:
        cp.wait()
    made = routing(id_ref[...], pj_ref[...], tok2[...], lax.rem(me["z"], 2))
    for k in range(8):
        mine[pl.ds(k, 1), :] = made[k]
        mg[me["y"], me["z"], pl.ds(k, 1), :] = made[k]
    here = mg.at[me["y"], me["z"]]
    mgot = [remote(mine, here, ms.at[k], mr.at[k], ring(me, "z", k + 1), sends) for k in range(3)]
    tok.second()
    eload = copy(emb_ref, emb, esem)
    raw.wait()

    def low(i, _):
        r = wraw[pl.ds(i * 4, 4)].reshape(16, 2880)
        for v in range(8):
            at = pl.ds(pl.multiple_of(i * 16, 16), 16)
            wd[v % 2, at, pl.ds((v // 2) * 384, 360)] = r[:, 360 * v : 360 * v + 360]
            wd[v % 2, at, pl.ds((v // 2) * 384 + 360, 24)] = jnp.zeros((16, 24), jnp.bfloat16)
        return 0

    lax.fori_loop(0, 45, low, 0)
    raw = copy(wg_ref, wraw, rawsem.at[1])
    for cp in mgot:
        cp.wait_recv()
    row = mg.at[me["y"]]
    mgot = [remote(row, row, ms.at[3 + k], mr.at[3 + k], ring(me, "y", k + 1), sends) for k in range(3)]
    tok.third()
    lead.second()
    raw.wait()

    def flat(dst):
        def body(i, _):
            dst[pl.ds(pl.multiple_of(i * 16, 16), 16), :] = wraw[pl.ds(i * 4, 4)].reshape(16, 2880)
            return 0

        lax.fori_loop(0, 45, body, 0)

    flat(wg)
    raw = copy(wu_ref, wraw, rawsem.at[2])
    tok.forward()
    lead.third()
    raw.wait()
    flat(wu)
    for cp in mgot:
        cp.wait_recv()
    base = ((me["y"] * 4 + me["z"]) * 32).astype(jnp.float32)
    for g in range(4):
        row = jnp.concatenate([mg[g, 0] + mg[g, 1], mg[g, 2] + mg[g, 3]], axis=1)
        hot, gate = plan(row, base)
        hots[g] = hot
        gates[pl.ds(128 * g, 128), :] = jnp.broadcast_to(gate, (128, 128))
    tok.last()
    tok.arrive()
    flat_tok = tg_ref.reshape(1024, 2880)
    loads = [copy(flat_tok.at[pl.ds(256 * g, 256)], rows.at[g], toksem.at[g]) for g in range(2)]
    for g in range(4):
        loads[g].wait()
        xs[pl.ds(128 * g, 128), :] = dot(hots[g], rows[g % 2], 1, 0).astype(jnp.bfloat16)
        if g < 2:
            loads.append(copy(flat_tok.at[pl.ds(256 * (g + 2), 256)], rows.at[g], toksem.at[g + 2]))
    lead.forward()
    for n0, n in ((0, 256), (256, 256), (512, 208)):
        gp = dot(xs[...], wg[pl.ds(n0, n), :], 1, 1)
        up = dot(xs[...], wu[pl.ds(n0, n), :], 1, 1)
        r = lax.broadcasted_iota(jnp.int32, (512, n), 0)
        q = lax.broadcasted_iota(jnp.int32, (512, n), 1)
        keep = lax.rem(lax.div(r, 8), 4) == lax.rem(q, 4)
        h = gp * jax.nn.sigmoid(1.702 * gp) * (up + 1.0)
        act[:, pl.ds(n0, n)] = jnp.where(keep, h, 0.0).astype(jnp.bfloat16)
    lead.last()

    hgot = []
    for half in range(2):
        side = 1 - c if half == 0 else c
        for xx in range(2):
            ys = dot(act[...], wd[side, :, pl.ds(768 * xx, 768)], 1, 0)
            for g in range(4):
                y = ys[128 * g : 128 * (g + 1)] * gates[pl.ds(128 * g, 128), pl.ds(0, 1)]
                high = y.astype(jnp.bfloat16)
                rest = (y - high.astype(jnp.float32)).astype(jnp.bfloat16)
                hot = hots[g]
                mix = dot(jnp.concatenate([hot, hot], axis=0), jnp.concatenate([high, rest], axis=0), 0, 0)
                for x in range(2):
                    for p in range(3):
                        piece = mix[:, 384 * x + 128 * p : 384 * x + 128 * (p + 1)].reshape(4, 64, 128)
                        if half == 0:
                            to_mate[p, 2 * xx + x, g] = piece.astype(jnp.bfloat16)
                        else:
                            own[p, 2 * xx + x, g] = piece
            if half == 0:
                part = pl.ds(2 * xx, 2)
                hgot.append(remote(to_mate.at[:, part], from_mate.at[:, part], hs.at[xx], hr.at[xx], mate, []))
    for cp in hgot:
        cp.wait()

    def index(p, at, full):
        return (p,) + tuple(at[d] if d in at else pl.ds(0, 4) for d in full)

    got1 = []
    for k in (1, 3, 2):
        for p in range(3):
            d = BACK[p][0]
            i = index(p, ring(me, d, k), DEST)
            to_mate[i] = (own[i] + from_mate[i].astype(jnp.float32)).astype(jnp.bfloat16)
            src = to_mate.at[i]
            got1.append((p, k, remote(src, in1.at[p, k - 1], s1.at[p, k - 1], r1.at[p, k - 1], ring(me, d, k), sends)))
    for p in range(3):
        i = index(p, {BACK[p][0]: me[BACK[p][0]]}, DEST)
        sum1[p] = own[i] + from_mate[i].astype(jnp.float32)

    lead.arrive()
    flat_rows = ag_ref.reshape(1024, 2880)
    xload = [copy(flat_rows.at[pl.ds(256 * i, 256)], rows.at[i], xsem.at[i]) for i in range(2)]
    eload.wait()
    stores = []

    def logits(j):
        xload[j].wait()
        inv = 1.0 / (0.5 + 0.25 * heat_ref[:, pl.ds(256 * j, 256)].astype(jnp.float32))
        if j >= 2:
            stores[j - 2].wait()
        buf = lg.at[j % 2]
        top = jnp.full((1, 256), -jnp.inf, jnp.float32)
        for i0, n in BLOCKS:
            r = dot(emb[pl.ds(i0, n), :], rows[j % 2], 1, 1) * inv
            buf[pl.ds(i0, n), :] = r
            top = jnp.maximum(top, jnp.max(r, axis=0, keepdims=True))
        if j < 2:
            xload.append(copy(flat_rows.at[pl.ds(256 * (j + 2), 256)], rows.at[j], xsem.at[j + 2]))

        def tail(i, s):
            return s + jnp.sum(jnp.exp(buf[pl.ds(pl.multiple_of(i * 112, 8), 112), :] - top), axis=0, keepdims=True)

        total = lax.fori_loop(0, 14, tail, jnp.zeros((1, 256), jnp.float32))
        total += jnp.sum(jnp.exp(buf[pl.ds(1568, 3), :] - top), axis=0, keepdims=True)
        for h in range(2):
            mb[0, 0, pl.ds(2 * j + h, 1), :] = top[:, 128 * h : 128 * (h + 1)]
            sb[0, 0, pl.ds(2 * j + h, 1), :] = total[:, 128 * h : 128 * (h + 1)]
        stores.append(copy(buf, sc_ref.at[:, pl.ds(256 * j, 256)], lsem.at[j]))

    stages = [[mate]] + [[ring(me, a, k) for k in range(1, 4)] for a in DEST]

    def begin(i):
        got = []
        for k, dev in enumerate(stages[i]):
            got.append(remote(mb.at[i, 0], mb.at[i, k + 1], ssem.at[0, i, k], rsem.at[0, i, k], dev, sends))
            got.append(remote(sb.at[i, 0], sb.at[i, k + 1], ssem.at[1, i, k], rsem.at[1, i, k], dev, sends))
        return got

    def end(i, got):
        for cp in got:
            cp.wait_recv()
        n = len(stages[i]) + 1
        top = mb[i, 0]
        for k in range(1, n):
            top = jnp.maximum(top, mb[i, k])
        total = sb[i, 0] * jnp.exp(mb[i, 0] - top)
        for k in range(1, n):
            total += sb[i, k] * jnp.exp(mb[i, k] - top)
        if i < 3:
            mb[i + 1, 0] = top
            sb[i + 1, 0] = total
        else:
            st_ref[...] = top + jnp.log(total)

    for j in range(3):
        logits(j)
    for p, k, cp in got1:
        cp.wait_recv()
        sum1[p] += in1[p, k - 1].astype(jnp.float32)
    got2 = []
    for p in range(3):
        d = BACK[p][1]
        first = [a for a in DEST if a != BACK[p][0]]
        for k in (1, 3, 2):
            i = index(p, ring(me, d, k), first)
            out2[p, k - 1] = sum1[i].astype(jnp.bfloat16)
            got2.append((p, k, remote(out2.at[p, k - 1], in2.at[p, k - 1], s2.at[p, k - 1], r2.at[p, k - 1], ring(me, d, k), sends)))
        sum2[p] = sum1[index(p, {d: me[d]}, first)]
    logits(3)
    got = begin(0)
    for p, k, cp in got2:
        cp.wait_recv()
        sum2[p] += in2[p, k - 1].astype(jnp.float32)
    got3 = []
    for p in range(3):
        d = BACK[p][2]
        for k in (1, 3, 2):
            out3[p, k - 1] = sum2[p, lax.rem(me[d] + k, 4)]
            got3.append(remote(out3.at[p, k - 1], in3.at[p, k - 1], s3.at[p, k - 1], r3.at[p, k - 1], ring(me, d, k), sends))
    end(0, got)
    got = begin(1)
    end(1, got)
    got = begin(2)
    for cp in got3:
        cp.wait_recv()
    for p in range(3):
        total = sum2[p, me[BACK[p][2]]]
        for k in range(3):
            total += in3[p, k]
        n = 128 if p < 2 else 104
        moe_ref[:, pl.ds(128 * p, n)] = total[:, :n].astype(jnp.bfloat16)
    end(2, got)
    got = begin(3)
    stores[2].wait()
    stores[3].wait()
    tok.drain()
    lead.drain()
    for cp in sends[: -len(got)]:
        cp.wait_send()
    end(3, got)
    for cp in got:
        cp.wait_send()


def main(tok, lead, ids, proj, heat, w_gate, w_up, w_down, embed):
    bf, f32 = jnp.bfloat16, jnp.float32
    dma = pltpu.SemaphoreType.DMA
    hbm = pl.BlockSpec(memory_space=pl.ANY)
    vm = pl.BlockSpec(memory_space=pltpu.VMEM)
    V = pltpu.VMEM
    return pl.pallas_call(
        main_kernel,
        out_shape=(
            jax.ShapeDtypeStruct((VOC, 1024), f32), jax.ShapeDtypeStruct((8, 128), f32),
            jax.ShapeDtypeStruct((64, 360), bf),
            jax.ShapeDtypeStruct((4, 2, 4, 4, 8, 2880), bf), jax.ShapeDtypeStruct((4, 4, 4, 2, 8, 2880), bf),
        ),
        in_specs=[hbm, hbm, vm, vm, vm, hbm, hbm, hbm, hbm],
        out_specs=[hbm, vm, vm, hbm, hbm],
        scratch_shapes=[
            V((720, 2880), bf), V((720, 2880), bf), V((180, 4, 2880), bf), V((2, 720, 1536), bf),
            V((8, 128), f32), V((4, 4, 8, 128), f32), V((2, 256, 2880), bf), V((512, 2880), bf), V((512, 720), bf),
            V((4, 128, 256), bf), V((512, 128), f32), V((128, 2880), bf),
            V((VOC, 2880), bf), V((2, VOC, 256), f32),
            V((3, 4, 4, 4, 64, 128), bf), V((3, 4, 4, 4, 64, 128), bf), V((3, 4, 4, 4, 64, 128), f32),
            V((3, 3, 4, 4, 64, 128), bf), V((3, 4, 4, 64, 128), f32),
            V((3, 3, 4, 64, 128), bf), V((3, 3, 4, 64, 128), bf), V((3, 4, 64, 128), f32),
            V((3, 3, 64, 128), f32), V((3, 3, 64, 128), f32),
            V((4, 4, 8, 128), f32), V((4, 4, 8, 128), f32),
        ]
        + [dma((3, 16))] * 4 + [dma((6,))] * 2 + [dma((4,)), dma((3,)), dma((4,)), dma, dma((4,)), dma((4,))]
        + [dma((2,))] * 2 + [dma((3, 3))] * 6 + [dma((2, 4, 3))] * 2,
        compiler_params=pltpu.CompilerParams(collective_id=0, has_side_effects=True, vmem_limit_bytes=67043328),
    )(tok, lead, ids, proj, heat, w_gate, w_up, w_down, embed)


STEPS = tuple((200 * i, 200 if i < 7 else 171) for i in range(8))


def last_kernel(s_ref, t_ref, o_ref, buf, isem, osem):
    loads = [copy(s_ref.at[pl.ds(i0, n)], buf.at[pl.ds(i0, n)], isem.at[i]) for i, (i0, n) in enumerate(STEPS)]
    outs = []
    for i, (i0, n) in enumerate(STEPS):
        loads[i].wait()
        buf[pl.ds(i0, n), :] = buf[pl.ds(i0, n), :] - t_ref[...]
        outs.append(copy(buf.at[pl.ds(i0, n)], o_ref.at[pl.ds(i0, n)], osem.at[i]))
    for cp in outs:
        cp.wait()


def last(scaled, shift):
    hbm = pl.BlockSpec(memory_space=pl.ANY)
    dma = pltpu.SemaphoreType.DMA
    return pl.pallas_call(
        last_kernel, out_shape=jax.ShapeDtypeStruct((VOC, 1024), jnp.float32),
        in_specs=[hbm, pl.BlockSpec(memory_space=pltpu.VMEM)], out_specs=hbm,
        scratch_shapes=[pltpu.VMEM((VOC, 1024), jnp.float32), dma((8,)), dma((8,))],
    )(scaled, shift)


def per_device(lead, heat, embed, tok, choice, proj, w_gate, w_up, w_down):
    flip = lambda w: jnp.transpose(w, (2, 0, 1))
    ids = choice.T
    scaled, shift, moe, _, _ = main(
        tok, lead, jnp.concatenate([ids, ids], axis=1), proj.T, heat.reshape(1, 1024),
        flip(w_gate), flip(w_up), jnp.transpose(w_down, (1, 0, 2)), embed,
    )
    return last(scaled, shift.reshape(1, 1024)).T, moe


def solution(mesh):
    torus = Mesh(mesh.devices.reshape(4, 2, 4, 4), AXES)
    placed = (
        P(AXES, None), P(), P(AXES, None), P(EXPERT, None), P(EXPERT, None), P(),
        P(EXPERT, None, VOCAB), P(EXPERT, None, VOCAB), P(EXPERT, VOCAB, None),
    )
    return jax.shard_map(
        per_device, mesh=torus, in_specs=placed,
        out_specs=(P(None, AXES), P(EXPERT, VOCAB)), check_vma=False,
    )
```

```python
import functools

import jax
import jax.numpy as jnp
from jax import lax
from jax.experimental import pallas as pl
from jax.experimental.pallas import tpu as pltpu
from jax.sharding import Mesh
from jax.sharding import PartitionSpec as P

AXES = ("x", "c", "y", "z")
EXPERT = ("y", "z")
VOCAB = ("x", "c")
MESH = pl.DeviceIdType.MESH
COLS = ((0, 1024), (1024, 1024), (2048, 832))
TCOLS = ((0, 640), (640, 1152), (1792, 1088))
ORDERS = (("z", "y", "x"), ("x", "z", "y"), ("x", "y", "z"))
EX, HOLD, SLOTS = 64, 4, 8


def ring(me, axis, step):
    return {axis: lax.rem(me[axis] + step, 4)}


def greet():
    me = {a: lax.axis_index(a) for a in AXES}
    barrier = pltpu.get_barrier_semaphore()
    for a in ("x", "y", "z"):
        for k in range(1, 4):
            pl.semaphore_signal(barrier, inc=1, device_id=ring(me, a, k), device_id_type=MESH)
    pl.semaphore_signal(barrier, inc=1, device_id={"c": 1 - me["c"]}, device_id_type=MESH)
    return me, barrier


def view(g, dims, me, ranges, cols, at={}):
    idx = [ranges.get(a, at.get(a, me[a])) for a in dims]
    return g.at[idx[0], idx[1], idx[2], idx[3], :, pl.ds(*cols)]


def remote(src, dst, ssem, rsem, dev, sends):
    cp = pltpu.make_async_remote_copy(
        src_ref=src, dst_ref=dst, send_sem=ssem, recv_sem=rsem, device_id=dev, device_id_type=MESH
    )
    cp.start()
    sends.append(cp)
    return cp


ALL = pl.ds(0, 4)


class Gather:
    def __init__(self, a, g, dims, cols, shared, me, ssem, rsem, own):
        self.dims, self.cols, self.shared = dims, cols, shared
        self.orders = ORDERS if shared else BACK
        self.a, self.g, self.me, self.ssem, self.rsem = a, g, me, ssem, rsem
        self.sends, self.mates, self.got, self.over = [], [], [None] * 3, [None] * 3
        x, c, y, z = (me[d] for d in AXES)
        if shared:
            n = cols[0][1]
            left, right = pl.ds(0, n), pl.ds(n, 2880 - n)
            self.own = [
                copy(a.at[x, c, :, left], g.at[y, z, x, c, :, left], own[0]),
                copy(a.at[:, c, :, right], g.at[y, z, :, c, :, right], own[1]),
            ]
        else:
            self.own = [copy(a, g.at[x, c, y, z], own[0])]

    def settle(self):
        for cp in self.own:
            cp.wait()

    def send(self, p, k, src, dst, dev):
        return remote(src, dst, self.ssem.at[p, k], self.rsem.at[p, k], dev, self.sends)

    def view(self, p, ranges, at={}):
        return view(self.g, self.dims, self.me, ranges, self.cols[p], at)

    def skips(self, p):
        return self.shared and self.orders[p][0] == "x"

    def first(self):
        me = self.me
        for p in range(3):
            d0, d1, _ = self.orders[p]
            if self.skips(p):
                src = self.a.at[:, me["c"], :, pl.ds(*self.cols[p])]
                dst = self.view(p, {d0: ALL})
                self.got[p] = [self.send(p, 2 + k, src, dst, ring(me, d1, k)) for k in (1, 3, 2)]
            else:
                src = self.a.at[me["x"], me["c"]] if self.shared else self.a
                src = src.at[:, pl.ds(*self.cols[p])]
                self.got[p] = [self.send(p, k - 1, src, self.view(p, {}), ring(me, d0, k)) for k in (1, 3, 2)]

    def second(self, p):
        for cp in self.got[p]:
            cp.wait_recv()
        d0, d1, _ = self.orders[p]
        blk = self.view(p, {d0: ALL})
        self.got[p] = [self.send(p, 2 + k, blk, blk, ring(self.me, d1, k)) for k in (1, 3, 2)]

    def mate(self, p, k, blk):
        self.mates.append(self.send(p, k, blk, blk, {"c": 1 - self.me["c"]}))

    def third(self, p):
        for cp in self.got[p]:
            cp.wait_recv()
        d0, d1, d2 = self.orders[p]
        halves = [self.view(p, {d0: pl.ds(2 * h, 2), d1: ALL}) for h in range(2)]
        self.got[p] = {}
        for o in range(2):
            for k, h in ((1, o), (3, 1 - o)):
                self.got[p][k, h] = self.send(p, 6 + 2 * (k // 2) + h, halves[h], halves[h], ring(self.me, d2, k))
        self.mate(p, 10, self.view(p, {d0: ALL, d1: ALL}))

    def forward(self, parts=(0, 1, 2)):
        for p in parts:
            d0, d1, d2 = self.orders[p]
            self.over[p] = []
            for k, h in ((1, 0), (3, 1)):
                self.got[p][k, h].wait_recv()
                half = self.view(p, {d0: pl.ds(2 * h, 2), d1: ALL}, ring(self.me, d2, 4 - k))
                self.over[p].append(self.send(p, 11 + h, half, half, ring(self.me, d2, k)))
        for p in parts:
            d0, d1, d2 = self.orders[p]
            for k, h in ((1, 0), (3, 1)):
                self.got[p][k, 1 - h].wait_recv()
                self.mate(p, 13 + h, self.view(p, {d0: ALL, d1: ALL}, ring(self.me, d2, 4 - k)))

    def last(self, parts=(0, 1, 2)):
        for p in parts:
            d0, d1, d2 = self.orders[p]
            for h in range(2):
                self.over[p][h].wait_recv()
            self.mate(p, 15, self.view(p, {d0: ALL, d1: ALL}, ring(self.me, d2, 2)))

    def arrive(self):
        for cp in self.mates:
            cp.wait_recv()

    def drain(self):
        for cp in self.sends:
            cp.wait_send()


def plan(meta_row, base):
    slot = lax.broadcasted_iota(jnp.int32, (128, 256), 0).astype(jnp.float32)
    src = (lax.broadcasted_iota(jnp.int32, (1, 256), 1) // 64).astype(jnp.float32) * 32.0
    hot = jnp.zeros((128, 256), jnp.float32)
    gates = jnp.zeros((128, 256), jnp.float32)
    for k in range(4):
        key = meta_row[k : k + 1] - base
        key = jnp.where((key >= 0.0) & (key < 32.0), key + src, -1.0)
        eq = slot == key
        hot += jnp.where(eq, 1.0, 0.0)
        gates += jnp.where(eq, meta_row[4 + k : 5 + k], 0.0)
    return hot.astype(jnp.bfloat16), jnp.sum(gates, axis=1, keepdims=True)


def copy(src, dst, sem):
    cp = pltpu.make_async_copy(src, dst, sem)
    cp.start()
    return cp


def dot(a, b, ca, cb):
    return lax.dot_general(a, b, (((ca,), (cb,)), ((), ())), preferred_element_type=jnp.float32)


BACK = (("z", "y", "x"), ("x", "z", "y"), ("y", "x", "z"))
DEST = ("x", "y", "z")
VOC = 1571
VMEM_LIMIT = 67043328
BLOCKS = ((0, 528), (528, 528), (1056, 515))


def routing(ids, proj, tok, odd):
    scores = dot(proj, tok, 1, 1)
    twice = lax.broadcasted_iota(jnp.int32, (64, 128), 0) == lax.rem(lax.broadcasted_iota(jnp.int32, (64, 128), 1), 64)
    ids = dot(ids.astype(jnp.float32).astype(jnp.bfloat16), twice.astype(jnp.float32).astype(jnp.bfloat16), 1, 0)
    expert = lax.broadcasted_iota(jnp.int32, (EX, 128), 0).astype(jnp.float32)
    hot = [(expert == ids[k : k + 1]).astype(jnp.float32) for k in range(4)]
    picked = [jnp.sum(h * scores, axis=0, keepdims=True) for h in hot]
    top = jnp.maximum(jnp.maximum(picked[0], picked[1]), jnp.maximum(picked[2], picked[3]))
    weights = [jnp.exp(p - top) for p in picked]
    total = weights[0] + weights[1] + weights[2] + weights[3]
    a = lax.broadcasted_iota(jnp.int32, (128, 128), 0)
    b = lax.broadcasted_iota(jnp.int32, (128, 128), 1)
    before = ((a < 64) & (a < lax.rem(b, 64))).astype(jnp.bfloat16)
    named = hot[0] + hot[1] + hot[2] + hot[3]
    earlier = dot(named.astype(jnp.bfloat16), before, 1, 0)
    lane = lax.broadcasted_iota(jnp.int32, (1, 128), 1)
    here = lax.div(lane, 64) == odd
    rows = []
    for k in range(4):
        slot = jnp.sum(hot[k] * earlier, axis=0, keepdims=True)
        rows.append(jnp.where(here, ids[k : k + 1] * SLOTS + slot, 0.0))
    for k in range(4):
        rows.append(jnp.where(here, weights[k] / total, 0.0))
    return rows


def main_kernel(
    t_ref, a_ref, id_ref, pj_ref, heat_ref, wg_ref, wu_ref, wd_ref, emb_ref,
    sc_ref, st_ref, moe_ref, ag_ref,
    stv, moev, tg, wg, wu, wraw, wd, mine, mg, rows, xs, act, hots, gates, tok2,
    emb, lg, to_mate, from_mate, own, in1, sum1, out2, in2, sum2, out3, in3, mb, sb,
    ts, tr, as_, ar, ms, mr, loc, rawsem, esem, xsem, lsem, osem,
    hs, hr, s1, r1, s2, r2, s3, r3, ssem, rsem,
):
    c = lax.axis_index("c")
    load = [copy(t_ref, tok2.at[pl.ds(64 * h, 64)], loc.at[2 + h]) for h in range(2)]
    chunks = [(w, i) for w in (wd_ref, wg_ref, wu_ref) for i in range(5)]
    raws = []

    def fetch(n):
        w, i = chunks[n]
        raws.append(copy(w.at[pl.ds(36 * i, 36)], wraw.at[n % 2], rawsem.at[n]))

    fetch(0)
    fetch(1)
    me, barrier = greet()
    for cp in load:
        cp.wait()
    made = routing(id_ref[...], pj_ref[...], tok2[...], lax.rem(me["z"], 2))
    for k in range(8):
        mine[pl.ds(k, 1), :] = made[k]
        mg[me["y"], me["z"], pl.ds(k, 1), :] = made[k]
    pl.semaphore_wait(barrier, 10)
    sends = []
    mate = {"c": 1 - me["c"]}
    here = mg.at[me["y"], me["z"]]
    mgot = [remote(mine, here, ms.at[k], mr.at[k], ring(me, "z", k + 1), sends) for k in range(3)]
    tok = Gather(t_ref.reshape(4, 2, 8, 2880), tg, ("y", "z", "x", "c"), TCOLS, True, me, ts, tr, (loc.at[0], loc.at[4]))
    tok.first()
    lead = Gather(a_ref, ag_ref, AXES, COLS, False, me, as_, ar, (loc.at[1],))
    lead.first()

    def relay(n):
        w, c0 = n // 5, 144 * (n % 5)
        raws[n].wait()

        def body(i, _):
            r = wraw[n % 2, pl.ds(i * 4, 4)].reshape(16, 2880)
            at = pl.ds(pl.multiple_of(c0 + i * 16, 16), 16)
            if w > 0:
                (wg, wu)[w - 1][at, :] = r
                return 0
            for v in range(8):
                wd[v % 2, at, pl.ds((v // 2) * 384, 360)] = r[:, 360 * v : 360 * v + 360]
                wd[v % 2, at, pl.ds((v // 2) * 384 + 360, 24)] = jnp.zeros((16, 24), jnp.bfloat16)
            return 0

        lax.fori_loop(0, 9, body, 0)
        if n + 2 < 15:
            fetch(n + 2)

    for n in range(2):
        relay(n)
    tok.settle()
    for cp in mgot:
        cp.wait_recv()
    row = mg.at[me["y"]]
    mgot = [remote(row, row, ms.at[3 + k], mr.at[3 + k], ring(me, "y", k + 1), sends) for k in range(3)]
    tok.second(0)
    tok.third(1)
    tok.third(2)
    lead.settle()
    for p in range(3):
        lead.second(p)
    for n in range(2, 4):
        relay(n)
    eload = copy(emb_ref, emb, esem)
    for n in range(4, 6):
        relay(n)
    tok.third(0)
    for n in range(6, 9):
        relay(n)
    tok.forward((1, 2))
    for n in range(9, 12):
        relay(n)
    tok.forward((0,))
    for p in range(3):
        lead.third(p)
    for n in range(12, 15):
        relay(n)
    for cp in mgot:
        cp.wait_recv()
    base = ((me["y"] * 4 + me["z"]) * 32).astype(jnp.float32)
    for g in range(4):
        row = jnp.concatenate([mg[g, 0] + mg[g, 1], mg[g, 2] + mg[g, 3]], axis=1)
        hot, gate = plan(row, base)
        hots[g] = hot
        gates[pl.ds(128 * g, 128), :] = jnp.broadcast_to(gate, (128, 128))
    tok.last((1, 2, 0))
    tok.arrive()
    tokens = tg.reshape(1024, 2880)
    for g in range(4):
        xs[pl.ds(128 * g, 128), :] = dot(hots[g], tokens[pl.ds(256 * g, 256), :], 1, 0).astype(jnp.bfloat16)
    for n0, n in ((0, 256), (256, 256), (512, 208)):
        gp = dot(xs[...], wg[pl.ds(n0, n), :], 1, 1)
        up = dot(xs[...], wu[pl.ds(n0, n), :], 1, 1)
        r = lax.broadcasted_iota(jnp.int32, (512, n), 0)
        q = lax.broadcasted_iota(jnp.int32, (512, n), 1)
        keep = lax.rem(lax.div(r, 8), 4) == lax.rem(q, 4)
        h = gp * jax.nn.sigmoid(1.702 * gp) * (up + 1.0)
        act[:, pl.ds(n0, n)] = jnp.where(keep, h, 0.0).astype(jnp.bfloat16)
        if n0 == 0:
            lead.forward()

    hgot, xload, stores = [], [], []
    flat_rows = ag_ref.reshape(1024, 2880)
    for half in range(2):
        side = 1 - c if half == 0 else c
        for xx in range(2):
            if half == 0 and xx == 1:
                lead.last()
            if half == 1 and xx == 1:
                lead.arrive()
                xload += [copy(flat_rows.at[pl.ds(256 * i, 256)], rows.at[i], xsem.at[i]) for i in range(2)]
                eload.wait()
            ys = dot(act[...], wd[side, :, pl.ds(768 * xx, 768)], 1, 0)
            for g in range(4):
                y = ys[128 * g : 128 * (g + 1)] * gates[pl.ds(128 * g, 128), pl.ds(0, 1)]
                high = y.astype(jnp.bfloat16)
                rest = (y - high.astype(jnp.float32)).astype(jnp.bfloat16)
                hot = hots[g]
                mix = dot(jnp.concatenate([hot, hot], axis=0), jnp.concatenate([high, rest], axis=0), 0, 0)
                for x in range(2):
                    for p in range(3):
                        piece = mix[:, 384 * x + 128 * p : 384 * x + 128 * (p + 1)].reshape(4, 64, 128)
                        if half == 0:
                            to_mate[p, 2 * xx + x, g] = piece.astype(jnp.bfloat16)
                        else:
                            own[p, 2 * xx + x, g] = piece
            if half == 0:
                part = pl.ds(2 * xx, 2)
                hgot.append(remote(to_mate.at[:, part], from_mate.at[:, part], hs.at[xx], hr.at[xx], mate, []))

    tops, sums = [], []

    def fold(x, f):
        n = x.shape[0] // 8 * 8
        return f(x[:n].reshape(n // 8, 8, x.shape[1]), axis=0)

    def expo(j, i0, n):
        return jnp.exp(lg[j % 2, pl.ds(i0, n), :] - tops[j])

    def logits(j):
        xload[j].wait()
        inv = 1.0 / (0.5 + 0.25 * heat_ref[:, pl.ds(256 * j, 256)].astype(jnp.float32))
        if j >= 2:
            stores[j - 2].wait()
        top = jnp.full((8, 256), -jnp.inf, jnp.float32)
        total = jnp.zeros((8, 256), jnp.float32)
        for i0, n in BLOCKS:
            r = dot(emb[pl.ds(i0, n), :], rows[j % 2], 1, 1) * inv
            lg[j % 2, pl.ds(i0, n), :] = r
            top = jnp.maximum(top, fold(r, jnp.max))
            if j > 0:
                total += fold(expo(j - 1, i0, n // 8 * 8), jnp.sum)
        if j > 0:
            sums.append(jnp.sum(total, axis=0, keepdims=True) + jnp.sum(expo(j - 1, 1568, 3), axis=0, keepdims=True))
        top = jnp.max(top, axis=0, keepdims=True)
        tops.append(jnp.maximum(top, jnp.max(lg[j % 2, pl.ds(1568, 3), :], axis=0, keepdims=True)))
        if j < 2:
            xload.append(copy(flat_rows.at[pl.ds(256 * (j + 2), 256)], rows.at[j], xsem.at[j + 2]))
        stores.append(copy(lg.at[j % 2], sc_ref.at[:, pl.ds(256 * j, 256)], lsem.at[j]))

    def put(j):
        for h in range(2):
            mb[0, 0, pl.ds(2 * j + h, 1), :] = tops[j][:, 128 * h : 128 * (h + 1)]
            sb[0, 0, pl.ds(2 * j + h, 1), :] = sums[j][:, 128 * h : 128 * (h + 1)]

    logits(0)
    for cp in hgot:
        cp.wait()

    def index(p, at, full):
        return (p,) + tuple(at[d] if d in at else pl.ds(0, 4) for d in full)

    got1 = []
    for k in (1, 3, 2):
        for p in range(3):
            d = BACK[p][0]
            i = index(p, ring(me, d, k), DEST)
            to_mate[i] = (own[i] + from_mate[i].astype(jnp.float32)).astype(jnp.bfloat16)
            src = to_mate.at[i]
            got1.append((p, k, remote(src, in1.at[p, k - 1], s1.at[p, k - 1], r1.at[p, k - 1], ring(me, d, k), sends)))
    for p in range(3):
        i = index(p, {BACK[p][0]: me[BACK[p][0]]}, DEST)
        sum1[p] = own[i] + from_mate[i].astype(jnp.float32)

    stages = [[mate]] + [[ring(me, a, k) for k in range(1, 4)] for a in DEST]

    def begin(i):
        got = []
        for k, dev in enumerate(stages[i]):
            got.append(remote(mb.at[i, 0], mb.at[i, k + 1], ssem.at[0, i, k], rsem.at[0, i, k], dev, sends))
            got.append(remote(sb.at[i, 0], sb.at[i, k + 1], ssem.at[1, i, k], rsem.at[1, i, k], dev, sends))
        return got

    def end(i, got):
        for cp in got:
            cp.wait_recv()
        n = len(stages[i]) + 1
        top = mb[i, 0]
        for k in range(1, n):
            top = jnp.maximum(top, mb[i, k])
        total = sb[i, 0] * jnp.exp(mb[i, 0] - top)
        for k in range(1, n):
            total += sb[i, k] * jnp.exp(mb[i, k] - top)
        if i < 3:
            mb[i + 1, 0] = top
            sb[i + 1, 0] = total
        else:
            stv[...] = top + jnp.log(total)

    for j in range(1, 4):
        logits(j)
        put(j - 1)
    total = jnp.zeros((8, 256), jnp.float32)
    for i0, n in BLOCKS:
        total += fold(expo(3, i0, n // 8 * 8), jnp.sum)
    sums.append(jnp.sum(total, axis=0, keepdims=True) + jnp.sum(expo(3, 1568, 3), axis=0, keepdims=True))
    put(3)
    got = begin(0)
    for p, k, cp in got1:
        cp.wait_recv()
        sum1[p] += in1[p, k - 1].astype(jnp.float32)
    rest = [[a for a in DEST if a != BACK[p][0]] for p in range(3)]
    for p in range(3):
        d = BACK[p][1]
        for k in (1, 3, 2):
            out2[p, k - 1] = sum1[index(p, ring(me, d, k), rest[p])].astype(jnp.bfloat16)
        sum2[p] = sum1[index(p, {d: me[d]}, rest[p])]
    end(0, got)
    got = begin(1)
    got2 = [
        (p, k, remote(out2.at[p, k - 1], in2.at[p, k - 1], s2.at[p, k - 1], r2.at[p, k - 1], ring(me, BACK[p][1], k), sends))
        for k in (1, 3, 2)
        for p in range(3)
    ]
    end(1, got)
    got = begin(2)
    for p, k, cp in got2:
        cp.wait_recv()
        sum2[p] += in2[p, k - 1].astype(jnp.float32)
    got3 = []
    for p in range(3):
        d = BACK[p][2]
        for k in (1, 3, 2):
            out3[p, k - 1] = sum2[p, lax.rem(me[d] + k, 4)]
            got3.append(remote(out3.at[p, k - 1], in3.at[p, k - 1], s3.at[p, k - 1], r3.at[p, k - 1], ring(me, d, k), sends))
    end(2, got)
    got = begin(3)
    tok.drain()
    lead.drain()
    for cp in stores[2:]:
        cp.wait()
    for cp in sends[: -len(got)]:
        cp.wait_send()
    for cp in got3:
        cp.wait_recv()
    for p in range(3):
        total = sum2[p, me[BACK[p][2]]]
        for k in range(3):
            total += in3[p, k]
        n = 128 if p < 2 else 104
        moev[:, pl.ds(128 * p, n)] = total[:, :n].astype(jnp.bfloat16)
    moe_out = copy(moev, moe_ref, osem.at[0])
    end(3, got)
    st_out = copy(stv, st_ref, osem.at[1])
    moe_out.wait()
    for cp in got:
        cp.wait_send()
    st_out.wait()


def main(tok, lead, ids, proj, heat, w_gate, w_up, w_down, embed):
    bf, f32 = jnp.bfloat16, jnp.float32
    dma = pltpu.SemaphoreType.DMA
    hbm = pl.BlockSpec(memory_space=pl.ANY)
    vm = pl.BlockSpec(memory_space=pltpu.VMEM)
    V = pltpu.VMEM
    return pl.pallas_call(
        main_kernel,
        out_shape=(
            jax.ShapeDtypeStruct((VOC, 1024), f32), jax.ShapeDtypeStruct((8, 128), f32),
            jax.ShapeDtypeStruct((64, 360), bf),
            jax.ShapeDtypeStruct((4, 2, 4, 4, 8, 2880), bf),
        ),
        in_specs=[hbm, hbm, vm, vm, vm, hbm, hbm, hbm, hbm],
        out_specs=[hbm, hbm, hbm, hbm],
        scratch_shapes=[
            V((8, 128), f32), V((64, 360), bf), V((4, 4, 4, 2, 8, 2880), bf), V((720, 2880), bf), V((720, 2880), bf), V((2, 36, 4, 2880), bf), V((2, 720, 1536), bf),
            V((8, 128), f32), V((4, 4, 8, 128), f32), V((2, 256, 2880), bf), V((512, 2880), bf), V((512, 720), bf),
            V((4, 128, 256), bf), V((512, 128), f32), V((128, 2880), bf),
            V((VOC, 2880), bf), V((2, VOC, 256), f32),
            V((3, 4, 4, 4, 64, 128), bf), V((3, 4, 4, 4, 64, 128), bf), V((3, 4, 4, 4, 64, 128), f32),
            V((3, 3, 4, 4, 64, 128), bf), V((3, 4, 4, 64, 128), f32),
            V((3, 3, 4, 64, 128), bf), V((3, 3, 4, 64, 128), bf), V((3, 4, 64, 128), f32),
            V((3, 3, 64, 128), f32), V((3, 3, 64, 128), f32),
            V((4, 4, 8, 128), f32), V((4, 4, 8, 128), f32),
        ]
        + [dma((3, 16))] * 4 + [dma((6,))] * 2 + [dma((5,)), dma((15,)), dma, dma((4,)), dma((4,)), dma((2,))]
        + [dma((2,))] * 2 + [dma((3, 3))] * 6 + [dma((2, 4, 3))] * 2,
        compiler_params=pltpu.CompilerParams(collective_id=0, has_side_effects=True, vmem_limit_bytes=VMEM_LIMIT),
    )(tok, lead, ids, proj, heat, w_gate, w_up, w_down, embed)


STEPS = tuple((200 * i, 200 if i < 7 else 171) for i in range(8))


def last_kernel(s_ref, t_ref, e_ref, o_ref, eo_ref, buf, ebuf, isem, osem, esem):
    loads = [copy(s_ref.at[pl.ds(i0, n)], buf.at[pl.ds(i0, n)], isem.at[i]) for i, (i0, n) in enumerate(STEPS)]
    small = copy(e_ref, ebuf, esem.at[0])
    outs = []
    for i, (i0, n) in enumerate(STEPS):
        loads[i].wait()
        if i == 4:
            small.wait()
            outs.append(copy(ebuf, eo_ref, esem.at[1]))
        buf[pl.ds(i0, n), :] = buf[pl.ds(i0, n), :] - t_ref[...]
        outs.append(copy(buf.at[pl.ds(i0, n)], o_ref.at[pl.ds(i0, n)], osem.at[i]))
    for cp in outs:
        cp.wait()


def last(scaled, shift, moe):
    hbm = pl.BlockSpec(memory_space=pl.ANY)
    vm = pl.BlockSpec(memory_space=pltpu.VMEM)
    dma = pltpu.SemaphoreType.DMA
    return pl.pallas_call(
        last_kernel, out_shape=(jax.ShapeDtypeStruct((VOC, 1024), jnp.float32), jax.ShapeDtypeStruct((64, 360), jnp.bfloat16)),
        in_specs=[hbm, vm, hbm], out_specs=[hbm, hbm],
        scratch_shapes=[pltpu.VMEM((VOC, 1024), jnp.float32), pltpu.VMEM((64, 360), jnp.bfloat16), dma((8,)), dma((8,)), dma((2,))],
        compiler_params=pltpu.CompilerParams(vmem_limit_bytes=67043328),
    )(scaled, shift, moe)


def per_device(lead, heat, embed, tok, choice, proj, w_gate, w_up, w_down):
    flip = lambda w: jnp.transpose(w, (2, 0, 1))
    scaled, shift, moe, _ = main(
        tok, lead, choice.T, proj.T, heat.reshape(1, 1024),
        flip(w_gate), flip(w_up), jnp.transpose(w_down, (1, 0, 2)), embed,
    )
    out, moe = last(scaled, shift.reshape(1, 1024), moe)
    return out.T, moe


def solution(mesh):
    torus = Mesh(mesh.devices.reshape(4, 2, 4, 4), AXES)
    placed = (
        P(AXES, None), P(), P(AXES, None), P(EXPERT, None), P(EXPERT, None), P(),
        P(EXPERT, None, VOCAB), P(EXPERT, None, VOCAB), P(EXPERT, VOCAB, None),
    )
    return jax.shard_map(
        per_device, mesh=torus, in_specs=placed,
        out_specs=(P(None, AXES), P(EXPERT, VOCAB)), check_vma=False,
    )
```
